32 devices in a mesh: dp: 32 (over z, y, x, core).
Axes of the slice: x: 2, y: 2, z: 4, core: 2. Of those that a mesh axis runs over, the one named last changes fastest.
Arguments:
- x_in: bfloat16 [32768, 1024], P('dp')
- dy_mid: bfloat16 [32768, 4096], P('dp')
- x_mid: bfloat16 [32768, 4096], P('dp')
- dy_out: bfloat16 [32768, 1024], P('dp')
- w_fc1: float32 [1024, 4096], replicated
- w_fc2: float32 [4096, 1024], replicated
- stat_left: float32 [32, 512, 512], P('dp')
- stat_right: float32 [32, 512, 512], P('dp')
- root_left: float32 [32, 512, 512], P('dp')
- root_right: float32 [32, 512, 512], P('dp')
- graft_sq: float32 [32, 512, 512], P('dp')
- momentum: float32 [32, 512, 512], P('dp')
Outputs:
- output 1: float32 [1024, 4096], replicated
- output 2: float32 [4096, 1024], replicated
- output 3: float32 [32, 512, 512], P('dp')
- output 4: float32 [32, 512, 512], P('dp')
- output 5: float32 [32, 512, 512], P('dp')
- output 6: float32 [32, 512, 512], P('dp')
All inputs are finite; a program needn't handle non-finite values.
Results may differ from the reference program's by a relative error of at most 0.001.
Values are sent between devices in bfloat16 or wider.
A program may use at most 1 GiB of HBM per device.

```python
import jax
import jax.numpy as jnp

D = 1024
FF = 4096
BLOCK = 512
TOKENS = 1024
DEVICES = 32
STEP = 10

ROW_BLOCKS = (D + BLOCK - 1) // BLOCK
COL_BLOCKS = (FF + BLOCK - 1) // BLOCK
HALF_BLOCKS = ROW_BLOCKS * COL_BLOCKS
NUM_BLOCKS = 2 * HALF_BLOCKS
ROWS_ALL = DEVICES * TOKENS
STAT_DECAY = 0.999
MOM_DECAY = 0.9
GRAFT_EPS = 1e-8
LEARN_RATE = 0.01
WEIGHT_DECAY = 1e-4
BIAS_CORR = 1.0 - STAT_DECAY ** STEP


def spd_draw(key_pair, low_diag, high_diag):
    diag_key, factor_key = jax.random.split(key_pair)
    diag_vals = jax.random.uniform(diag_key, (NUM_BLOCKS, BLOCK), jnp.float32, low_diag, high_diag)
    factor = jax.random.normal(factor_key, (NUM_BLOCKS, BLOCK, 64), jnp.float32)
    low_rank = jnp.einsum('nik,njk->nij', factor, factor) / 128.0
    return low_rank + diag_vals[:, :, None] * jnp.eye(BLOCK, dtype=jnp.float32)


def setup_inputs(seed: int = 0) -> dict:
    key_list = jax.random.split(jax.random.key(seed), 12)
    grad_scale = TOKENS ** -0.5
    stat_scale = 0.01 * BLOCK / DEVICES
    x_in = jax.random.normal(key_list[0], (ROWS_ALL, D), jnp.float32).astype(jnp.bfloat16)
    dy_mid = (jax.random.normal(key_list[1], (ROWS_ALL, FF), jnp.float32) * grad_scale).astype(jnp.bfloat16)
    x_mid = jax.random.normal(key_list[2], (ROWS_ALL, FF), jnp.float32).astype(jnp.bfloat16)
    dy_out = (jax.random.normal(key_list[3], (ROWS_ALL, D), jnp.float32) * grad_scale).astype(jnp.bfloat16)
    w_fc1 = jax.random.normal(key_list[4], (D, FF), jnp.float32) * D ** -0.5
    w_fc2 = jax.random.normal(key_list[5], (FF, D), jnp.float32) * FF ** -0.5
    stat_left = stat_scale * spd_draw(key_list[6], 0.2, 1.0)
    stat_right = stat_scale * spd_draw(key_list[7], 0.2, 1.0)
    root_left = spd_draw(key_list[8], 0.2, 1.0)
    root_right = spd_draw(key_list[9], 0.2, 1.0)
    graft_sq = (BIAS_CORR / DEVICES) * jax.random.uniform(key_list[10], (NUM_BLOCKS, BLOCK, BLOCK), jnp.float32, 0.2, 2.0)
    momentum = jax.random.normal(key_list[11], (NUM_BLOCKS, BLOCK, BLOCK), jnp.float32)
    return {'x_in': x_in, 'dy_mid': dy_mid, 'x_mid': x_mid, 'dy_out': dy_out, 'w_fc1': w_fc1, 'w_fc2': w_fc2, 'stat_left': stat_left, 'stat_right': stat_right, 'root_left': root_left, 'root_right': root_right, 'graft_sq': graft_sq, 'momentum': momentum}


def to_blocks(matrix, row_blocks, col_blocks):
    padded = jnp.pad(matrix, ((0, row_blocks * BLOCK - matrix.shape[0]), (0, col_blocks * BLOCK - matrix.shape[1])))
    return padded.reshape(row_blocks, BLOCK, col_blocks, BLOCK).transpose(0, 2, 1, 3).reshape(row_blocks * col_blocks, BLOCK, BLOCK)


def from_blocks(blocks, row_blocks, col_blocks, n_rows, n_cols):
    full_mat = blocks.reshape(row_blocks, col_blocks, BLOCK, BLOCK).transpose(0, 2, 1, 3)
    return full_mat.reshape(row_blocks * BLOCK, col_blocks * BLOCK)[:n_rows, :n_cols]


def keep_mask(block_ids):
    is_first = block_ids < HALF_BLOCKS
    local_ids = block_ids % HALF_BLOCKS
    row_first = jnp.minimum(D - (local_ids // COL_BLOCKS) * BLOCK, BLOCK)
    col_first = jnp.minimum(FF - (local_ids % COL_BLOCKS) * BLOCK, BLOCK)
    row_second = jnp.minimum(FF - (local_ids // ROW_BLOCKS) * BLOCK, BLOCK)
    col_second = jnp.minimum(D - (local_ids % ROW_BLOCKS) * BLOCK, BLOCK)
    row_count = jnp.where(is_first, row_first, row_second)
    col_count = jnp.where(is_first, col_first, col_second)
    offsets = jnp.arange(BLOCK)
    return (offsets[None, :, None] < row_count[:, None, None]) & (offsets[None, None, :] < col_count[:, None, None])


def reference(x_in, dy_mid, x_mid, dy_out, w_fc1, w_fc2, stat_left, stat_right, root_left, root_right, graft_sq, momentum):
    grad_fc1 = jnp.dot(x_in.T, dy_mid, preferred_element_type=jnp.float32) / DEVICES
    grad_fc2 = jnp.dot(x_mid.T, dy_out, preferred_element_type=jnp.float32) / DEVICES
    grad_blk = jnp.concatenate([to_blocks(grad_fc1, ROW_BLOCKS, COL_BLOCKS), to_blocks(grad_fc2, COL_BLOCKS, ROW_BLOCKS)], axis=0)
    new_left = STAT_DECAY * stat_left + (1.0 - STAT_DECAY) * jnp.einsum('nik,njk->nij', grad_blk, grad_blk)
    new_right = STAT_DECAY * stat_right + (1.0 - STAT_DECAY) * jnp.einsum('nki,nkj->nij', grad_blk, grad_blk)
    precond = jnp.einsum('nij,njk->nik', jnp.einsum('nij,njk->nik', root_left, grad_blk), root_right)
    precond = jnp.where(keep_mask(jnp.arange(NUM_BLOCKS)), precond, 0.0)
    new_sq = STAT_DECAY * graft_sq + (1.0 - STAT_DECAY) * grad_blk * grad_blk
    graft_dir = grad_blk / (jnp.sqrt(new_sq / BIAS_CORR) + GRAFT_EPS)
    graft_norm = jnp.sqrt(jnp.sum(graft_dir * graft_dir, axis=(1, 2)))
    pre_norm = jnp.sqrt(jnp.sum(precond * precond, axis=(1, 2)))
    new_mom = MOM_DECAY * momentum + precond * (graft_norm / pre_norm)[:, None, None]
    direction = new_mom.astype(jnp.bfloat16).astype(jnp.float32)
    dir_fc1 = from_blocks(direction[:HALF_BLOCKS], ROW_BLOCKS, COL_BLOCKS, D, FF)
    dir_fc2 = from_blocks(direction[HALF_BLOCKS:], COL_BLOCKS, ROW_BLOCKS, FF, D)
    new_w1 = w_fc1 - LEARN_RATE * (dir_fc1 + WEIGHT_DECAY * w_fc1)
    new_w2 = w_fc2 - LEARN_RATE * (dir_fc2 + WEIGHT_DECAY * w_fc2)
    return (new_w1, new_w2, new_left, new_right, new_sq, new_mom)
```

```python
import functools

import jax
import jax.numpy as jnp
from jax import lax
from jax.experimental import pallas as pl
from jax.experimental.pallas import tpu as pltpu
from jax.sharding import PartitionSpec as P

STEP = 10
STAT_DECAY = 0.999
MOM_DECAY = 0.9
GRAFT_EPS = 1e-8
LEARN_RATE = 0.01
WEIGHT_DECAY = 1e-4
BIAS_CORR = 1.0 - STAT_DECAY ** STEP

MESH = pl.DeviceIdType.MESH
HOPS = (2, 3, 1, 0)
GATHER_HOPS = (0, 1, 3, 2)


def dev(z, y, x, c):
    return (((z * 2 + y) * 2 + x) * 2 + c,)


def coords():
    me = lax.axis_index("dp")
    return me // 8, (me // 4) % 2, (me // 2) % 2, me % 2


def greet(z, y, x, c):
    barrier = pltpu.get_barrier_semaphore()
    peers = [dev(z, y, 1 - x, c), dev(z, 1 - y, x, c), dev(z, y, x, 1 - c)]
    peers += [dev((z + k) % 4, y, x, c) for k in (1, 2, 3)]
    for peer in peers:
        pl.semaphore_signal(barrier, inc=1, device_id=peer, device_id_type=MESH)
    pl.semaphore_wait(barrier, len(peers))


def remote(src, dst, send_sem, recv_sem, peer):
    return pltpu.make_async_remote_copy(src_ref=src, dst_ref=dst, send_sem=send_sem, recv_sem=recv_sem, device_id=peer, device_id_type=MESH)


def reduce_kernel(x_in, dy_mid, x_mid, dy_out, out_ref, xi, dm, xm, do, acc, rx, ry, rz, lsem, psem, qsem, xs, xr, ys, yr, zs, zr, osem):
    z, y, x, c = coords()
    rows = x_in.shape[0]
    bd = 512
    half = bd // 2
    xp, yp, cp = dev(z, y, 1 - x, c), dev(z, 1 - y, x, c), dev(z, y, x, 1 - c)
    own = y * 2 + x

    def cols(i):
        return pl.ds(pl.multiple_of(i * bd, bd), bd)

    def operand(kind, i):
        if kind == "xi":
            return i, x_in.at[:, cols(i)], x_in.at[:, cols(i)], xi.at[i]
        if kind == "dm":
            return 2 + i, dy_mid.at[:, cols(2 * i + c)], dy_mid.at[:, cols(2 * i + 1 - c)], dm.at[i]
        if kind == "xm":
            return 6 + i, x_mid.at[:, cols(i)], x_mid.at[:, cols(i)], xm.at[i]
        return 14, dy_out.at[:, cols(c)], dy_out.at[:, cols(1 - c)], do

    def here(kind, i):
        s, mine, _, dst = operand(kind, i)
        return pltpu.make_async_copy(mine, dst.at[pl.ds(0, rows)], lsem.at[s])

    def there(kind, i):
        s, _, theirs, dst = operand(kind, i)
        return remote(theirs, dst.at[pl.ds(rows, rows)], qsem.at[s], psem.at[s], cp)

    def fetch(kind, i):
        there(kind, i).start()
        here(kind, i).start()

    def arrive(kind, i):
        here(kind, i).wait()
        there(kind, i).wait_recv()

    greet(z, y, x, c)

    zb = [(z + h) % 4 for h in HOPS]
    first1 = [zb[0] < 2, (zb[1] < 2) & (zb[0] >= 2)]
    first2 = [zb[0] >= 2, (zb[1] >= 2) & (zb[0] < 2)]
    first1 += [(zb[2] < 2) & (zb[0] >= 2) & (zb[1] >= 2), zb[0] < 0]
    first2 += [(zb[2] >= 2) & (zb[0] < 2) & (zb[1] < 2), zb[0] < 0]
    order = [(1 - y) * 2 + 1 - x, y * 2 + 1 - x, (1 - y) * 2 + x, own]

    for k in range(4):
        @pl.when(zb[k] < 2)
        def _():
            fetch("xi", zb[k])

        @pl.when(first2[k])
        def _():
            fetch("do", 0)

        for q in range(4):
            @pl.when(first1[k])
            def _():
                fetch("dm", order[q])

            @pl.when(zb[k] >= 2)
            def _():
                fetch("xm", (zb[k] - 2) * 4 + order[q])

    def dots(lhs, rhs, dst):
        for h in range(2):
            dst[h] = lax.dot_general(lhs[:, h * half:(h + 1) * half], rhs[...], (((0,), (0,)), ((), ())), preferred_element_type=jnp.float32)

    def send_one(k, q, j):
        @pl.when(q < 2)
        def _():
            remote(acc.at[k, j, 0], rx.at[k, q], xs.at[k, q], xr.at[k, q], xp).start()

        @pl.when(q % 2 == 0)
        def _():
            remote(acc.at[k, j, 1], ry.at[k, q // 2], ys.at[k, q // 2], yr.at[k, q // 2], yp).start()

    def pick(values, i):
        out = values[-1]
        for n in range(len(values) - 2, -1, -1):
            out = jnp.where(i == n, values[n], out)
        return out

    def group(k, _):
        zk = pick(zb, k)
        f1, f2 = pick([v.astype(jnp.int32) for v in first1], k), pick([v.astype(jnp.int32) for v in first2], k)

        @pl.when(zk < 2)
        def _():
            arrive("xi", zk)

        @pl.when(f2 == 1)
        def _():
            arrive("do", 0)

        def tile(q, _):
            j = pick(order, q)

            @pl.when(f1 == 1)
            def _():
                arrive("dm", j)

            @pl.when(zk < 2)
            def _():
                dots(xi.at[zk], dm.at[j], acc.at[k, j])

            @pl.when(zk >= 2)
            def _():
                t = (zk - 2) * 4 + j
                arrive("xm", t)
                dots(xm.at[t], do, acc.at[k, j])

            @pl.when(k < 2)
            def _():
                send_one(k, q, j)

            return 0

        return lax.fori_loop(0, 4, tile, 0)

    lax.fori_loop(0, 4, group, 0)

    def add(k, j, h, ref):
        acc[k, j, h] += ref[...]

    def got(buf, ss, rs, k, i):
        remote(buf.at[k, i], buf.at[k, i], ss.at[k, i], rs.at[k, i], xp).wait_recv()

    def start_one(k):
        for q in range(3):
            if q < 2:
                remote(acc.at[k, order[q], 0], rx.at[k, q], xs.at[k, q], xr.at[k, q], xp).start()
            if q % 2 == 0:
                remote(acc.at[k, order[q], 1], ry.at[k, q // 2], ys.at[k, q // 2], yr.at[k, q // 2], yp).start()

    def start_two(k):
        got(rx, xs, xr, k, 0)
        add(k, order[2], 0, rx.at[k, 0])
        remote(acc.at[k, order[2], 0], ry.at[k, 2], ys.at[k, 2], yr.at[k, 2], yp).start()
        got(ry, ys, yr, k, 0)
        add(k, order[1], 1, ry.at[k, 0])
        remote(acc.at[k, order[1], 1], rx.at[k, 2], xs.at[k, 2], xr.at[k, 2], xp).start()

    def finish_plane(k):
        got(rx, xs, xr, k, 1)
        add(k, own, 0, rx.at[k, 1])
        got(ry, ys, yr, k, 1)
        add(k, own, 1, ry.at[k, 1])
        for h, (buf, ss, rs) in enumerate(((ry, ys, yr), (rx, xs, xr))):
            got(buf, ss, rs, k, 2)
            add(k, own, h, buf.at[k, 2])
            if k < 3:
                remote(acc.at[k, own, h], rz.at[k, h], zs.at[k, h], zr.at[k, h], dev(zb[k], y, x, c)).start()

    start_two(0)
    start_one(2)
    start_two(1)
    finish_plane(0)
    start_two(2)
    start_one(3)
    finish_plane(1)
    finish_plane(2)
    start_two(3)
    finish_plane(3)

    for k in range(3):
        for h in range(2):
            remote(rz.at[k, h], rz.at[k, h], zs.at[k, h], zr.at[k, h], xp).wait_recv()
            add(3, own, h, rz.at[k, h])
    outs = []
    for h in range(2):
        acc[3, own, h] = acc[3, own, h] * (1.0 / 32.0)
        o = pltpu.make_async_copy(acc.at[3, own, h], out_ref.at[pl.ds(h * half, half)], osem.at[h])
        o.start()
        outs.append(o)
    for s in range(15):
        kind, i = ("xi", s) if s < 2 else ("dm", s - 2) if s < 6 else ("xm", s - 6) if s < 14 else ("do", 0)
        there(kind, i).wait_send()
    for k in range(4):
        for i in range(3):
            remote(rx.at[k, i], rx.at[k, i], xs.at[k, i], xr.at[k, i], xp).wait_send()
            remote(ry.at[k, i], ry.at[k, i], ys.at[k, i], yr.at[k, i], yp).wait_send()
    for k in range(3):
        for h in range(2):
            remote(rz.at[k, h], rz.at[k, h], zs.at[k, h], zr.at[k, h], xp).wait_send()
    for o in outs:
        o.wait()


def reduce_gradients(x_in, dy_mid, x_mid, dy_out):
    bf, f32 = jnp.bfloat16, jnp.float32
    rows = 2 * x_in.shape[0]
    dma = pltpu.SemaphoreType.DMA
    any_spec = pl.BlockSpec(memory_space=pl.ANY)
    return pl.pallas_call(
        reduce_kernel,
        out_shape=jax.ShapeDtypeStruct((512, 512), f32),
        in_specs=[any_spec] * 4,
        out_specs=any_spec,
        scratch_shapes=[
            pltpu.VMEM((2, rows, 512), bf), pltpu.VMEM((4, rows, 512), bf), pltpu.VMEM((8, rows, 512), bf), pltpu.VMEM((rows, 512), bf),
            pltpu.VMEM((4, 4, 2, 256, 512), f32), pltpu.VMEM((4, 3, 256, 512), f32), pltpu.VMEM((4, 3, 256, 512), f32), pltpu.VMEM((3, 2, 256, 512), f32),
            dma((15,)), dma((15,)), dma((15,)), dma((4, 3)), dma((4, 3)), dma((4, 3)), dma((4, 3)), dma((3, 2)), dma((3, 2)), dma((2,)),
        ],
        compiler_params=pltpu.CompilerParams(collective_id=0, has_side_effects=True, vmem_limit_bytes=67043328),
        name="reduce",
    )(x_in, dy_mid, x_mid, dy_out)


def gather_kernel(dir_ref, d1, d2, buf, isem, zs, zr, xs, xr, ys, yr, xds, xdr, yds, ydr, cs, cr, osem):
    z, y, x, c = coords()
    xp, yp, cp = dev(z, y, 1 - x, c), dev(z, 1 - y, x, c), dev(z, y, x, 1 - c)

    def blk(zb, yb, xb, cb):
        return dev(zb, yb, xb, cb)[0]

    bring = pltpu.make_async_copy(dir_ref, buf.at[blk(z, y, x, c)], isem)
    bring.start()
    greet(z, y, x, c)
    bring.wait()

    zb = [(z + 4 - h) % 4 for h in GATHER_HOPS]
    spots = [(y, x), (1 - y, x), (y, 1 - x), (1 - y, 1 - x)]

    def put(b, zk, n):
        def one():
            return pltpu.make_async_copy(buf.at[b], d1.at[pl.ds(pl.multiple_of((b // 8) * 512, 512), 512), pl.ds(pl.multiple_of((b % 8) * 512, 512), 512)], osem.at[n])

        def two():
            return pltpu.make_async_copy(buf.at[b], d2.at[pl.ds(pl.multiple_of(((b - 16) // 2) * 512, 512), 512), pl.ds(pl.multiple_of((b % 2) * 512, 512), 512)], osem.at[n])

        @pl.when(zk < 2)
        def _():
            one().start()

        @pl.when(zk >= 2)
        def _():
            two().start()

    def whole(ref, b):
        return ref.at[b]

    def part(ref, b, h):
        return ref.at[b, pl.ds(h * 256, 256)]

    def xcopy(k, b):
        return remote(buf.at[b], buf.at[b], xs.at[k], xr.at[k], xp)

    def ycopy(k, b):
        return remote(buf.at[b], buf.at[b], ys.at[k], yr.at[k], yp)

    def xdiag(k, b):
        return remote(part(buf, b, 0), part(buf, b, 0), xds.at[k], xdr.at[k], xp)

    def ydiag(k, b):
        return remote(part(buf, b, 1), part(buf, b, 1), yds.at[k], ydr.at[k], yp)

    def ccopy(k, i, b):
        return remote(buf.at[b], buf.at[b], cs.at[k, i], cr.at[k, i], cp)

    def zcopy(k, b, peer):
        return remote(buf.at[b], buf.at[b], zs.at[k - 1], zr.at[k - 1], peer)

    def open_group(k):
        b = blk(zb[k], y, x, c)
        xcopy(k, b).start()
        ycopy(k, b).start()
        ccopy(k, 0, b).start()
        put(b, zb[k], k * 8)

    b0 = blk(z, y, x, c)
    xcopy(0, b0).start()
    ycopy(0, b0).start()
    for k in (1, 2, 3):
        zcopy(k, b0, dev((z + GATHER_HOPS[k]) % 4, y, x, c)).start()
    ccopy(0, 0, b0).start()
    put(b0, z, 0)
    for k in range(4):
        by, bx, bd = [blk(zb[k], yy, xx, c) for yy, xx in spots[1:]]
        ycopy(k, by).wait_recv()
        xdiag(k, by).start()
        ccopy(k, 1, by).start()
        put(by, zb[k], k * 8 + 1)
        xcopy(k, bx).wait_recv()
        ydiag(k, bx).start()
        ccopy(k, 2, bx).start()
        put(bx, zb[k], k * 8 + 2)
        if k < 3:
            zcopy(k + 1, blk(zb[k + 1], y, x, c), xp).wait_recv()
            open_group(k + 1)
        xdiag(k, bd).wait_recv()
        ydiag(k, bd).wait_recv()
        ccopy(k, 3, bd).start()
        put(bd, zb[k], k * 8 + 3)
        for i, (yy, xx) in enumerate(spots):
            bo = blk(zb[k], yy, xx, 1 - c)
            ccopy(k, i, bo).wait_recv()
            put(bo, zb[k], k * 8 + 4 + i)
    for k in range(4):
        xcopy(k, b0).wait_send()
        ycopy(k, b0).wait_send()
        xdiag(k, b0).wait_send()
        ydiag(k, b0).wait_send()
        for i in range(4):
            ccopy(k, i, b0).wait_send()
        if k:
            zcopy(k, b0, xp).wait_send()
    for n in range(32):
        pltpu.make_async_copy(buf.at[0], d1.at[pl.ds(0, 512), pl.ds(0, 512)], osem.at[n]).wait()


def gather_directions(own_dir):
    bf = jnp.bfloat16
    dma = pltpu.SemaphoreType.DMA
    any_spec = pl.BlockSpec(memory_space=pl.ANY)
    return pl.pallas_call(
        gather_kernel,
        out_shape=(jax.ShapeDtypeStruct((1024, 4096), bf), jax.ShapeDtypeStruct((4096, 1024), bf)),
        in_specs=[any_spec],
        out_specs=(any_spec, any_spec),
        scratch_shapes=[pltpu.VMEM((32, 512, 512), bf), dma, dma((3,)), dma((3,))] + [dma((4,))] * 8 + [dma((4, 4)), dma((4, 4)), dma((32,))],
        compiler_params=pltpu.CompilerParams(collective_id=1, has_side_effects=True, vmem_limit_bytes=40 * 2 ** 20),
        name="gather",
    )(own_dir)


def mm(a, b):
    return jnp.dot(a, b, precision=lax.Precision.HIGHEST, preferred_element_type=jnp.float32)


def solution(mesh):
    def per_device(x_in, dy_mid, x_mid, dy_out, w_fc1, w_fc2, stat_left, stat_right, root_left, root_right, graft_sq, momentum):
        grad = reduce_gradients(x_in, dy_mid, x_mid, dy_out)
        precond = mm(mm(root_left[0], grad), root_right[0])
        new_sq = STAT_DECAY * graft_sq[0] + (1.0 - STAT_DECAY) * grad * grad
        graft_dir = grad / (jnp.sqrt(new_sq / BIAS_CORR) + GRAFT_EPS)
        graft_norm = jnp.sqrt(jnp.sum(graft_dir * graft_dir))
        pre_norm = jnp.sqrt(jnp.sum(precond * precond))
        new_mom = MOM_DECAY * momentum[0] + precond * (graft_norm / pre_norm)
        dir1, dir2 = gather_directions(new_mom.astype(jnp.bfloat16))
        new_left = STAT_DECAY * stat_left[0] + (1.0 - STAT_DECAY) * mm(grad, grad.T)
        new_right = STAT_DECAY * stat_right[0] + (1.0 - STAT_DECAY) * mm(grad.T, grad)
        new_w1 = w_fc1 - LEARN_RATE * (dir1.astype(jnp.float32) + WEIGHT_DECAY * w_fc1)
        new_w2 = w_fc2 - LEARN_RATE * (dir2.astype(jnp.float32) + WEIGHT_DECAY * w_fc2)
        return new_w1, new_w2, new_left[None], new_right[None], new_sq[None], new_mom[None]

    row_spec = P('dp', None)
    rep_spec = P(None, None)
    tile_spec = P('dp', None, None)
    in_specs = (row_spec, row_spec, row_spec, row_spec, rep_spec, rep_spec, tile_spec, tile_spec, tile_spec, tile_spec, tile_spec, tile_spec)
    out_specs = (rep_spec, rep_spec, tile_spec, tile_spec, tile_spec, tile_spec)
    return jax.shard_map(per_device, mesh=mesh, in_specs=in_specs, out_specs=out_specs, check_vma=False)
```

```python
import functools

import jax
import jax.numpy as jnp
from jax import lax
from jax.experimental import pallas as pl
from jax.experimental.pallas import tpu as pltpu
from jax.sharding import PartitionSpec as P

STEP = 10
STAT_DECAY = 0.999
MOM_DECAY = 0.9
GRAFT_EPS = 1e-8
LEARN_RATE = 0.01
WEIGHT_DECAY = 1e-4
BIAS_CORR = 1.0 - STAT_DECAY ** STEP

MESH = pl.DeviceIdType.MESH
HOPS = (2, 3, 1, 0)
GATHER_HOPS = (0, 1, 3, 2)


def dev(z, y, x, c):
    return (((z * 2 + y) * 2 + x) * 2 + c,)


def coords():
    me = lax.axis_index("dp")
    return me // 8, (me // 4) % 2, (me // 2) % 2, me % 2


def greet_signal(z, y, x, c):
    peers = [dev(z, y, 1 - x, c), dev(z, 1 - y, x, c), dev(z, y, x, 1 - c)]
    peers += [dev((z + k) % 4, y, x, c) for k in (1, 2, 3)]
    for peer in peers:
        pl.semaphore_signal(pltpu.get_barrier_semaphore(), inc=1, device_id=peer, device_id_type=MESH)


def greet_wait():
    pl.semaphore_wait(pltpu.get_barrier_semaphore(), 6)


def remote(src, dst, send_sem, recv_sem, peer):
    return pltpu.make_async_remote_copy(src_ref=src, dst_ref=dst, send_sem=send_sem, recv_sem=recv_sem, device_id=peer, device_id_type=MESH)


def reduce_kernel(x_in, dy_mid, x_mid, dy_out, out_ref, xi, dm, xm, do, acc, rx, ry, rz, lsem, psem, qsem, xs, xr, ys, yr, zs, zr, osem):
    z, y, x, c = coords()
    rows = x_in.shape[0]
    bd = 512
    half = bd // 2
    xp, yp, cp = dev(z, y, 1 - x, c), dev(z, 1 - y, x, c), dev(z, y, x, 1 - c)
    own = y * 2 + x

    def cols(i):
        return pl.ds(pl.multiple_of(i * bd, bd), bd)

    def operand(kind, i):
        if kind == "xi":
            return i, x_in.at[:, cols(i)], x_in.at[:, cols(i)], xi.at[i]
        if kind == "dm":
            return 2 + i, dy_mid.at[:, cols(2 * i + c)], dy_mid.at[:, cols(2 * i + 1 - c)], dm.at[i]
        if kind == "xm":
            return 6 + i, x_mid.at[:, cols(i)], x_mid.at[:, cols(i)], xm.at[i]
        return 14, dy_out.at[:, cols(c)], dy_out.at[:, cols(1 - c)], do

    def here(kind, i):
        s, mine, _, dst = operand(kind, i)
        return pltpu.make_async_copy(mine, dst.at[pl.ds(0, rows)], lsem.at[s])

    def there(kind, i):
        s, _, theirs, dst = operand(kind, i)
        return remote(theirs, dst.at[pl.ds(rows, rows)], qsem.at[s], psem.at[s], cp)

    def fetch(kind, i):
        there(kind, i).start()
        here(kind, i).start()

    def arrive(kind, i):
        here(kind, i).wait()
        there(kind, i).wait_recv()

    greet_signal(z, y, x, c)
    greet_wait()

    zb = [(z + h) % 4 for h in HOPS]
    first1 = [zb[0] < 2, (zb[1] < 2) & (zb[0] >= 2)]
    first2 = [zb[0] >= 2, (zb[1] >= 2) & (zb[0] < 2)]
    first1 += [(zb[2] < 2) & (zb[0] >= 2) & (zb[1] >= 2), zb[0] < 0]
    first2 += [(zb[2] >= 2) & (zb[0] < 2) & (zb[1] < 2), zb[0] < 0]
    order = [(1 - y) * 2 + 1 - x, y * 2 + 1 - x, (1 - y) * 2 + x, own]

    for k in range(4):
        @pl.when(zb[k] < 2)
        def _():
            fetch("xi", zb[k])

        @pl.when(first2[k])
        def _():
            fetch("do", 0)

        for q in range(4):
            @pl.when(first1[k])
            def _():
                fetch("dm", order[q])

            @pl.when(zb[k] >= 2)
            def _():
                fetch("xm", (zb[k] - 2) * 4 + order[q])

    def dots(lhs, rhs, dst):
        for h in range(2):
            dst[h] = lax.dot_general(lhs[:, h * half:(h + 1) * half], rhs[...], (((0,), (0,)), ((), ())), preferred_element_type=jnp.float32)

    def send_one(k, q, j):
        @pl.when(q < 2)
        def _():
            remote(acc.at[k, j, 0], rx.at[k, q], xs.at[k, q], xr.at[k, q], xp).start()

        @pl.when(q % 2 == 0)
        def _():
            remote(acc.at[k, j, 1], ry.at[k, q // 2], ys.at[k, q // 2], yr.at[k, q // 2], yp).start()

    def pick(values, i):
        out = values[-1]
        for n in range(len(values) - 2, -1, -1):
            out = jnp.where(i == n, values[n], out)
        return out

    def group(k, _):
        zk = pick(zb, k)
        f1, f2 = pick([v.astype(jnp.int32) for v in first1], k), pick([v.astype(jnp.int32) for v in first2], k)

        @pl.when(zk < 2)
        def _():
            arrive("xi", zk)

        @pl.when(f2 == 1)
        def _():
            arrive("do", 0)

        def tile(q, _):
            j = pick(order, q)

            @pl.when(f1 == 1)
            def _():
                arrive("dm", j)

            @pl.when(zk < 2)
            def _():
                dots(xi.at[zk], dm.at[j], acc.at[k, j])

            @pl.when(zk >= 2)
            def _():
                t = (zk - 2) * 4 + j
                arrive("xm", t)
                dots(xm.at[t], do, acc.at[k, j])

            @pl.when(k < 2)
            def _():
                send_one(k, q, j)

            return 0

        return lax.fori_loop(0, 4, tile, 0)

    lax.fori_loop(0, 4, group, 0)

    def add(k, j, h, ref):
        acc[k, j, h] += ref[...]

    def got(buf, ss, rs, k, i):
        remote(buf.at[k, i], buf.at[k, i], ss.at[k, i], rs.at[k, i], xp).wait_recv()

    def start_one(k):
        for q in range(3):
            if q < 2:
                remote(acc.at[k, order[q], 0], rx.at[k, q], xs.at[k, q], xr.at[k, q], xp).start()
            if q % 2 == 0:
                remote(acc.at[k, order[q], 1], ry.at[k, q // 2], ys.at[k, q // 2], yr.at[k, q // 2], yp).start()

    def start_two(k):
        got(rx, xs, xr, k, 0)
        add(k, order[2], 0, rx.at[k, 0])
        remote(acc.at[k, order[2], 0], ry.at[k, 2], ys.at[k, 2], yr.at[k, 2], yp).start()
        got(ry, ys, yr, k, 0)
        add(k, order[1], 1, ry.at[k, 0])
        remote(acc.at[k, order[1], 1], rx.at[k, 2], xs.at[k, 2], xr.at[k, 2], xp).start()

    def finish_plane(k):
        got(rx, xs, xr, k, 1)
        add(k, own, 0, rx.at[k, 1])
        got(ry, ys, yr, k, 1)
        add(k, own, 1, ry.at[k, 1])
        for h, (buf, ss, rs) in enumerate(((ry, ys, yr), (rx, xs, xr))):
            got(buf, ss, rs, k, 2)
            add(k, own, h, buf.at[k, 2])
            if k < 3:
                remote(acc.at[k, own, h], rz.at[k, h], zs.at[k, h], zr.at[k, h], dev(zb[k], y, x, c)).start()

    start_two(0)
    start_one(2)
    start_two(1)
    finish_plane(0)
    start_two(2)
    start_one(3)
    finish_plane(1)
    finish_plane(2)
    start_two(3)
    finish_plane(3)

    for k in range(3):
        for h in range(2):
            remote(rz.at[k, h], rz.at[k, h], zs.at[k, h], zr.at[k, h], xp).wait_recv()
            add(3, own, h, rz.at[k, h])
    outs = []
    for h in range(2):
        acc[3, own, h] = acc[3, own, h] * (1.0 / 32.0)
        o = pltpu.make_async_copy(acc.at[3, own, h], out_ref.at[pl.ds(h * half, half)], osem.at[h])
        o.start()
        outs.append(o)
    for s in range(15):
        kind, i = ("xi", s) if s < 2 else ("dm", s - 2) if s < 6 else ("xm", s - 6) if s < 14 else ("do", 0)
        there(kind, i).wait_send()
    for k in range(4):
        for i in range(3):
            remote(rx.at[k, i], rx.at[k, i], xs.at[k, i], xr.at[k, i], xp).wait_send()
            remote(ry.at[k, i], ry.at[k, i], ys.at[k, i], yr.at[k, i], yp).wait_send()
    for k in range(3):
        for h in range(2):
            remote(rz.at[k, h], rz.at[k, h], zs.at[k, h], zr.at[k, h], xp).wait_send()
    for o in outs:
        o.wait()


def reduce_gradients(x_in, dy_mid, x_mid, dy_out):
    bf, f32 = jnp.bfloat16, jnp.float32
    rows = 2 * x_in.shape[0]
    dma = pltpu.SemaphoreType.DMA
    any_spec = pl.BlockSpec(memory_space=pl.ANY)
    return pl.pallas_call(
        reduce_kernel,
        out_shape=jax.ShapeDtypeStruct((512, 512), f32),
        in_specs=[any_spec] * 4,
        out_specs=any_spec,
        scratch_shapes=[
            pltpu.VMEM((2, rows, 512), bf), pltpu.VMEM((4, rows, 512), bf), pltpu.VMEM((8, rows, 512), bf), pltpu.VMEM((rows, 512), bf),
            pltpu.VMEM((4, 4, 2, 256, 512), f32), pltpu.VMEM((4, 3, 256, 512), f32), pltpu.VMEM((4, 3, 256, 512), f32), pltpu.VMEM((3, 2, 256, 512), f32),
            dma((15,)), dma((15,)), dma((15,)), dma((4, 3)), dma((4, 3)), dma((4, 3)), dma((4, 3)), dma((3, 2)), dma((3, 2)), dma((2,)),
        ],
        compiler_params=pltpu.CompilerParams(collective_id=0, has_side_effects=True, vmem_limit_bytes=67043328),
        name="reduce",
    )(x_in, dy_mid, x_mid, dy_out)


def gather_kernel(grad_in, rl_in, rr_in, sq_in, mom_in, sl_in, sr_in, w1_in, w2_in, new_left, new_right, new_sq, new_mom, w,
                  buf, grad, rl, rr, pre, isem, zs, zr, xs, xr, ys, yr, xds, xdr, yds, ydr, cs, cr):
    z, y, x, c = coords()
    xp, yp, cp = dev(z, y, 1 - x, c), dev(z, 1 - y, x, c), dev(z, y, x, 1 - c)

    def blk(zb, yb, xb, cb):
        return dev(zb, yb, xb, cb)[0]

    pairs = [(grad_in, grad), (rl_in, rl), (rr_in, rr), (sq_in, new_sq), (mom_in, new_mom), (sl_in, new_left), (sr_in, new_right), (w2_in, w.at[pl.ds(4096, 4096)])]
    pairs += [(w1_in.at[:, pl.ds(1024 * n, 1024)], w.at[pl.ds(1024 * n, 1024)]) for n in range(4)]
    loads = [pltpu.make_async_copy(src, dst, isem.at[i]) for i, (src, dst) in enumerate(pairs)]
    for load in loads[:5]:
        load.start()
    greet_signal(z, y, x, c)

    b0 = blk(z, y, x, c)
    for load in loads[:4]:
        load.wait()
    for load in loads[5:]:
        load.start()
    pre[...] = mm(rl[...], grad[...])
    rl[...] = mm(pre[...], rr[...])

    def strip_of(i):
        return pl.ds(pl.multiple_of(i * 64, 64), 64)

    def norms(i, sums):
        r = strip_of(i)
        g, p = grad[r], rl[r]
        sq = STAT_DECAY * new_sq[r] + (1.0 - STAT_DECAY) * g * g
        new_sq[r] = sq
        h = g / (jnp.sqrt(sq / BIAS_CORR) + GRAFT_EPS)
        return sums[0] + jnp.sum(h * h), sums[1] + jnp.sum(p * p)

    graft_sum, pre_sum = lax.fori_loop(0, 8, norms, (jnp.float32(0.0), jnp.float32(0.0)))
    loads[4].wait()
    ones = jnp.ones((64, 512), jnp.float32)
    scale = jnp.sqrt(graft_sum * ones) / jnp.sqrt(pre_sum * ones)

    def momentum_step(i, _):
        r = strip_of(i)
        mom = MOM_DECAY * new_mom[r] + rl[r] * scale
        new_mom[r] = mom
        buf[b0, r] = mom.astype(jnp.bfloat16)
        return 0

    lax.fori_loop(0, 8, momentum_step, 0)
    greet_wait()

    zb = [(z + 4 - h) % 4 for h in GATHER_HOPS]
    spots = [(y, x), (1 - y, x), (y, 1 - x), (1 - y, 1 - x)]

    def step(w, b, row, col):
        def strip(i, _):
            r = pl.ds(pl.multiple_of(row * 512 + i * 64, 64), 64)
            cc = pl.ds(pl.multiple_of(col * 512, 512), 512)
            old = w[r, cc]
            d = buf[b, pl.ds(pl.multiple_of(i * 64, 64), 64), :].astype(jnp.float32)
            w[r, cc] = old - LEARN_RATE * (d + WEIGHT_DECAY * old)
            return 0

        lax.fori_loop(0, 8, strip, 0)

    def apply(b, zk):
        first = zk < 2
        col = jnp.where(first, b % 8, b % 2)
        step(w, b, jnp.where(first, (col // 2) * 2 + b // 8, 8 + (b - 16) // 2), col % 2)

    def part(ref, b, h):
        return ref.at[b, pl.ds(h * 256, 256)]

    def xcopy(k, b):
        return remote(buf.at[b], buf.at[b], xs.at[k], xr.at[k], xp)

    def ycopy(k, b):
        return remote(buf.at[b], buf.at[b], ys.at[k], yr.at[k], yp)

    def xdiag(k, b):
        return remote(part(buf, b, 0), part(buf, b, 0), xds.at[k], xdr.at[k], xp)

    def ydiag(k, b):
        return remote(part(buf, b, 1), part(buf, b, 1), yds.at[k], ydr.at[k], yp)

    def ccopy(k, i, b):
        return remote(buf.at[b], buf.at[b], cs.at[k, i], cr.at[k, i], cp)

    def zcopy(k, b, peer):
        return remote(buf.at[b], buf.at[b], zs.at[k - 1], zr.at[k - 1], peer)

    xcopy(0, b0).start()
    ycopy(0, b0).start()
    for k in (1, 2, 3):
        zcopy(k, b0, dev((z + GATHER_HOPS[k]) % 4, y, x, c)).start()
    ccopy(0, 0, b0).start()
    for load in loads[5:7]:
        load.wait()
    pre[...] = mm(grad[...], grad[...], ((1,), (1,)))
    rr[...] = mm(grad[...], grad[...], ((0,), (0,)))

    def stats(i, _):
        r = strip_of(i)
        new_left[r] = STAT_DECAY * new_left[r] + (1.0 - STAT_DECAY) * pre[r]
        new_right[r] = STAT_DECAY * new_right[r] + (1.0 - STAT_DECAY) * rr[r]
        return 0

    lax.fori_loop(0, 8, stats, 0)
    for load in loads[7:]:
        load.wait()
    for k in range(4):
        b, by, bx, bd = [blk(zb[k], yy, xx, c) for yy, xx in spots]
        others = [blk(zb[k], yy, xx, 1 - c) for yy, xx in spots]
        ycopy(k, by).wait_recv()
        xdiag(k, by).start()
        ccopy(k, 1, by).start()
        xcopy(k, bx).wait_recv()
        ydiag(k, bx).start()
        ccopy(k, 2, bx).start()
        if k < 3:
            nb = blk(zb[k + 1], y, x, c)
            zcopy(k + 1, nb, xp).wait_recv()
            xcopy(k + 1, nb).start()
            ycopy(k + 1, nb).start()
            ccopy(k + 1, 0, nb).start()
        for t in (b, by, bx):
            apply(t, zb[k])
        for i in range(3):
            ccopy(k, i, others[i]).wait_recv()
            apply(others[i], zb[k])
        xdiag(k, bd).wait_recv()
        ydiag(k, bd).wait_recv()
        ccopy(k, 3, bd).start()
        apply(bd, zb[k])
        ccopy(k, 3, others[3]).wait_recv()
        apply(others[3], zb[k])
    for k in range(4):
        xcopy(k, b0).wait_send()
        ycopy(k, b0).wait_send()
        xdiag(k, b0).wait_send()
        ydiag(k, b0).wait_send()
        for i in range(4):
            ccopy(k, i, b0).wait_send()
        if k:
            zcopy(k, b0, xp).wait_send()


def finish_step(grad, root_left, root_right, graft_sq, momentum, stat_left, stat_right, w_fc1, w_fc2):
    bf, f32 = jnp.bfloat16, jnp.float32
    dma = pltpu.SemaphoreType.DMA
    any_spec = pl.BlockSpec(memory_space=pl.ANY)
    vmem_spec = pl.BlockSpec(memory_space=pltpu.VMEM)
    tile = pltpu.VMEM((512, 512), f32)
    return pl.pallas_call(
        gather_kernel,
        out_shape=(tile, tile, tile, tile, pltpu.VMEM((8192, 1024), f32)),
        in_specs=[any_spec] * 9,
        out_specs=(vmem_spec,) * 5,
        scratch_shapes=[pltpu.VMEM((32, 512, 512), bf)] + [pltpu.VMEM((512, 512), f32)] * 4 + [dma((12,)), dma((3,)), dma((3,))] + [dma((4,))] * 8 + [dma((4, 4)), dma((4, 4))],
        compiler_params=pltpu.CompilerParams(collective_id=1, has_side_effects=True, vmem_limit_bytes=26 * 2 ** 20),
        name="gather",
    )(grad, root_left, root_right, graft_sq, momentum, stat_left, stat_right, w_fc1, w_fc2)


def flush_kernel(left, right, sq, mom, w, left_out, right_out, sq_out, mom_out, w1_out, w2_out, sem):
    pairs = [(w.at[pl.ds(1024 * n, 1024)], w1_out.at[:, pl.ds(1024 * n, 1024)]) for n in range(4)]
    pairs += [(w.at[pl.ds(4096, 4096)], w2_out), (left, left_out), (right, right_out), (sq, sq_out), (mom, mom_out)]
    out = [pltpu.make_async_copy(src, dst, sem.at[i]) for i, (src, dst) in enumerate(pairs)]
    for o in out:
        o.start()
    for o in out:
        o.wait()


def flush(left, right, sq, mom, w, shape1, shape2):
    any_spec = pl.BlockSpec(memory_space=pl.ANY)
    tile = jax.ShapeDtypeStruct(left.shape, left.dtype)
    values = [pltpu.with_memory_space_constraint(v, pltpu.VMEM) for v in (left, right, sq, mom, w)]
    return pl.pallas_call(
        flush_kernel,
        out_shape=(tile, tile, tile, tile, jax.ShapeDtypeStruct(shape1, w.dtype), jax.ShapeDtypeStruct(shape2, w.dtype)),
        in_specs=[pl.BlockSpec(memory_space=pltpu.VMEM)] * 5,
        out_specs=(any_spec,) * 6,
        scratch_shapes=[pltpu.SemaphoreType.DMA((9,))],
        compiler_params=pltpu.CompilerParams(vmem_limit_bytes=2 ** 20),
        name="flush",
    )(*values)


def mm(a, b, dims=((1,), (0,))):
    return lax.dot_general(a, b, (dims, ((), ())), precision=lax.Precision.HIGHEST, preferred_element_type=jnp.float32)


def solution(mesh):
    def per_device(x_in, dy_mid, x_mid, dy_out, w_fc1, w_fc2, stat_left, stat_right, root_left, root_right, graft_sq, momentum):
        grad = reduce_gradients(x_in, dy_mid, x_mid, dy_out)
        done = finish_step(grad, root_left[0], root_right[0], graft_sq[0], momentum[0], stat_left[0], stat_right[0], w_fc1, w_fc2)
        new_left, new_right, new_sq, new_mom, new_w1, new_w2 = flush(*done, w_fc1.shape, w_fc2.shape)
        return new_w1, new_w2, new_left[None], new_right[None], new_sq[None], new_mom[None]

    row_spec = P('dp', None)
    rep_spec = P(None, None)
    tile_spec = P('dp', None, None)
    in_specs = (row_spec, row_spec, row_spec, row_spec, rep_spec, rep_spec, tile_spec, tile_spec, tile_spec, tile_spec, tile_spec, tile_spec)
    out_specs = (rep_spec, rep_spec, tile_spec, tile_spec, tile_spec, tile_spec)
    return jax.shard_map(per_device, mesh=mesh, in_specs=in_specs, out_specs=out_specs, check_vma=False)
```

```python
import functools

import jax
import jax.numpy as jnp
from jax import lax
from jax.experimental import pallas as pl
from jax.experimental.pallas import tpu as pltpu
from jax.sharding import PartitionSpec as P

STEP = 10
STAT_DECAY = 0.999
MOM_DECAY = 0.9
GRAFT_EPS = 1e-8
LEARN_RATE = 0.01
WEIGHT_DECAY = 1e-4
BIAS_CORR = 1.0 - STAT_DECAY ** STEP

MESH = pl.DeviceIdType.MESH
HOPS = (3, 2, 1, 0)
PLANE = 208
LINE = 512 - 2 * PLANE
GATHER_HOPS = (0, 1, 3, 2)


def dev(z, y, x, c):
    return (((z * 2 + y) * 2 + x) * 2 + c,)


def coords():
    me = lax.axis_index("dp")
    return me // 8, (me // 4) % 2, (me // 2) % 2, me % 2


def greet_signal(z, y, x, c):
    peers = [dev(z, y, 1 - x, c), dev(z, 1 - y, x, c), dev(z, y, x, 1 - c)]
    peers += [dev((z + k) % 4, y, x, c) for k in (1, 2, 3)]
    for peer in peers:
        pl.semaphore_signal(pltpu.get_barrier_semaphore(), inc=1, device_id=peer, device_id_type=MESH)


def greet_wait():
    pl.semaphore_wait(pltpu.get_barrier_semaphore(), 6)


def remote(src, dst, send_sem, recv_sem, peer):
    return pltpu.make_async_remote_copy(src_ref=src, dst_ref=dst, send_sem=send_sem, recv_sem=recv_sem, device_id=peer, device_id_type=MESH)


def reduce_kernel(x_in, dy_mid, x_mid, dy_out, out_ref, xi, dm, xm, do, acc, rx, ry, rx3, ry3, rz, ro, ri, lsem, psem, qsem, xs, xr, ys, yr, zs, zr, ls, lr, ms, mr, osem):
    z, y, x, c = coords()
    rows = x_in.shape[0]
    bd = 512
    half = bd // 2
    xp, yp, cp = dev(z, y, 1 - x, c), dev(z, 1 - y, x, c), dev(z, y, x, 1 - c)
    own = y * 2 + x

    def cols(i):
        return pl.ds(pl.multiple_of(i * bd, bd), bd)

    def operand(kind, i):
        if kind == "xi":
            return i, x_in.at[:, cols(i)], x_in.at[:, cols(i)], xi.at[i]
        if kind == "dm":
            return 2 + i, dy_mid.at[:, cols(2 * i + c)], dy_mid.at[:, cols(2 * i + 1 - c)], dm.at[i]
        if kind == "xm":
            return 6 + i, x_mid.at[:, cols(i)], x_mid.at[:, cols(i)], xm.at[i]
        return 14, dy_out.at[:, cols(c)], dy_out.at[:, cols(1 - c)], do

    def here(kind, i):
        s, mine, _, dst = operand(kind, i)
        return pltpu.make_async_copy(mine, dst.at[pl.ds(0, rows)], lsem.at[s])

    def there(kind, i):
        s, _, theirs, dst = operand(kind, i)
        return remote(theirs, dst.at[pl.ds(rows, rows)], qsem.at[s], psem.at[s], cp)

    def fetch(kind, i):
        there(kind, i).start()
        here(kind, i).start()

    def arrive(kind, i):
        here(kind, i).wait()
        there(kind, i).wait_recv()

    greet_signal(z, y, x, c)
    greet_wait()

    low = z < 2
    end = (z == 0) | (z == 3)
    hop = [jnp.where(low, h, (4 - h) % 4) for h in HOPS]
    zb = [(z + h) % 4 for h in hop]
    inner = dev(jnp.where(low, z + 1, z - 1), y, x, c)
    outer = dev(jnp.where(low, 0, 3), y, x, c)
    far = dev(jnp.where(low, 3, 0), y, x, c)
    first1 = [zb[0] < 2, (zb[1] < 2) & (zb[0] >= 2)]
    first2 = [zb[0] >= 2, (zb[1] >= 2) & (zb[0] < 2)]
    first1 += [(zb[2] < 2) & (zb[0] >= 2) & (zb[1] >= 2), zb[0] < 0]
    first2 += [(zb[2] >= 2) & (zb[0] < 2) & (zb[1] < 2), zb[0] < 0]
    order = [(1 - y) * 2 + 1 - x, y * 2 + 1 - x, (1 - y) * 2 + x, own]

    for k in range(4):
        @pl.when(zb[k] < 2)
        def _():
            fetch("xi", zb[k])

        @pl.when(first2[k])
        def _():
            fetch("do", 0)

        for q in range(4):
            @pl.when(first1[k])
            def _():
                fetch("dm", order[q])

            @pl.when(zb[k] >= 2)
            def _():
                fetch("xm", (zb[k] - 2) * 4 + order[q])

    def dots(lhs, rhs, dst):
        for h in range(2):
            dst[h * half:(h + 1) * half] = lax.dot_general(lhs[:, h * half:(h + 1) * half], rhs[...], (((0,), (0,)), ((), ())), preferred_element_type=jnp.float32)

    def size(k):
        return half if k == 3 else PLANE

    def rows_of(k, h):
        return pl.ds(h * size(k), size(k))

    def slot_x(k, i):
        return rx3.at[i] if k == 3 else rx.at[k, i]

    def slot_y(k, i):
        return ry3.at[i] if k == 3 else ry.at[k, i]

    def send_x(k, i, j, h):
        return remote(acc.at[k, j, rows_of(k, h)], slot_x(k, i), xs.at[k, i], xr.at[k, i], xp)

    def send_y(k, i, j, h):
        return remote(acc.at[k, j, rows_of(k, h)], slot_y(k, i), ys.at[k, i], yr.at[k, i], yp)

    def send_one(q, j):
        @pl.when(q < 2)
        def _():
            remote(acc.at[0, j, rows_of(0, 0)], rx.at[0, q], xs.at[0, q], xr.at[0, q], xp).start()

        @pl.when(q % 2 == 0)
        def _():
            remote(acc.at[0, j, rows_of(0, 1)], ry.at[0, q // 2], ys.at[0, q // 2], yr.at[0, q // 2], yp).start()

    line = pl.ds(2 * PLANE, LINE)

    def inward(k, n, q):
        return remote(acc.at[k, order_of(q), line], ro.at[n, q], ls.at[n, q], lr.at[n, q], inner)

    def across(k, n, q, peer):
        return remote(acc.at[k, order_of(q), line], ri.at[n, q], ms.at[n, q], mr.at[n, q], peer)

    def order_of(q):
        return order[q] if isinstance(q, int) else pick(order, q)

    def pass_on(n, q):
        inward(0, n, q).wait_recv()
        acc[n + 1, order_of(q), line] += ro[n, q]
        across(n + 1, n, q, inner).start()

    def pick(values, i):
        out = values[-1]
        for n in range(len(values) - 2, -1, -1):
            out = jnp.where(i == n, values[n], out)
        return out

    def group(k, _):
        zk = pick(zb, k)
        f1, f2 = pick([v.astype(jnp.int32) for v in first1], k), pick([v.astype(jnp.int32) for v in first2], k)

        @pl.when(zk < 2)
        def _():
            arrive("xi", zk)

        @pl.when(f2 == 1)
        def _():
            arrive("do", 0)

        def tile(q, _):
            j = pick(order, q)

            @pl.when(f1 == 1)
            def _():
                arrive("dm", j)

            @pl.when(zk < 2)
            def _():
                dots(xi.at[zk], dm.at[j], acc.at[k, j])

            @pl.when(zk >= 2)
            def _():
                t = (zk - 2) * 4 + j
                arrive("xm", t)
                dots(xm.at[t], do, acc.at[k, j])

            @pl.when(k < 1)
            def _():
                send_one(q, j)

            @pl.when(end & (k < 3))
            def _():
                inward(k, k, q).start()

            @pl.when(jnp.logical_not(end) & (k == 2))
            def _():
                pass_on(0, q)

            return 0

        return lax.fori_loop(0, 4, tile, 0)

    lax.fori_loop(0, 2, group, 0)

    def add(k, j, where, ref):
        acc[k, j, where] += ref[...]

    def start_one(k):
        send_x(k, 0, order[0], 0).start()
        send_y(k, 0, order[0], 1).start()
        send_x(k, 1, order[1], 0).start()
        send_y(k, 1, order[2], 1).start()

    def start_two(k):
        send_x(k, 0, own, 0).wait_recv()
        add(k, order[2], rows_of(k, 0), slot_x(k, 0))
        send_y(k, 2, order[2], 0).start()
        send_y(k, 0, own, 1).wait_recv()
        add(k, order[1], rows_of(k, 1), slot_y(k, 0))
        send_x(k, 2, order[1], 1).start()

    def send_z(k, h):
        n = jnp.where(end, k, (0, 1, 3)[k])
        peer = (jnp.where(end, inner[0], (outer, far, inner)[k][0]),)
        return remote(acc.at[k, own, rows_of(k, h)], rz.at[n, h], zs.at[k, h], zr.at[n, h], peer)

    def got_z(n, h):
        remote(rz.at[n, h], rz.at[n, h], zs.at[0, h], zr.at[n, h], inner).wait_recv()

    def relay(k):
        @pl.when(jnp.logical_not(end))
        def _():
            for h in range(2):
                got_z(k - 1, h)
                add(k, own, rows_of(k, h), rz.at[k - 1, h])
                send_z(k, h).start()

    def leave(k, h):
        if k == 0:
            send_z(k, h).start()
        elif k < 3:
            @pl.when(end)
            def _():
                send_z(k, h).start()

    def finish_plane(k):
        send_x(k, 1, own, 0).wait_recv()
        add(k, own, rows_of(k, 0), slot_x(k, 1))
        send_y(k, 1, own, 1).wait_recv()
        add(k, own, rows_of(k, 1), slot_y(k, 1))
        send_y(k, 2, own, 0).wait_recv()
        add(k, own, rows_of(k, 0), slot_y(k, 2))
        leave(k, 0)
        send_x(k, 2, own, 1).wait_recv()
        add(k, own, rows_of(k, 1), slot_x(k, 2))
        leave(k, 1)

    def line_first(n):
        @pl.when(jnp.logical_not(end))
        def _():
            for q in range(4):
                pass_on(n, q)

    def line_second():
        @pl.when(jnp.logical_not(end))
        def _():
            for q in range(4):
                across(0, 0, q, inner).wait_recv()
                add(0, order[q], line, ri.at[0, q])
                remote(acc.at[0, order[q], line], ri.at[0, q], ms.at[2, q], mr.at[0, q], outer).start()

    def line_last():
        @pl.when(end)
        def _():
            for q in range(4):
                across(0, 0, q, inner).wait_recv()
                add(3, order[q], line, ri.at[0, q])

        @pl.when(jnp.logical_not(end))
        def _():
            for q in range(4):
                inward(0, 2, q).wait_recv()
                add(3, order[q], line, ro.at[2, q])
                across(0, 1, q, inner).wait_recv()
                add(3, order[q], line, ri.at[1, q])

    start_two(0)
    start_one(1)
    lax.fori_loop(2, 4, group, 0)
    finish_plane(0)
    start_two(1)
    start_one(2)
    line_first(1)
    line_second()
    finish_plane(1)
    start_two(2)
    line_last()
    start_one(3)
    relay(1)
    finish_plane(2)
    start_two(3)
    relay(2)
    finish_plane(3)

    for n in range(2):
        for h in range(2):
            slot = jnp.where(end, n, n + 2)
            got_z(slot, h)
            add(3, own, rows_of(0, h), rz.at[slot, h])
    outs = []
    for h in range(2):
        part = pl.ds(h * half, half)
        acc[3, own, part] = acc[3, own, part] * (1.0 / 32.0)
        o = pltpu.make_async_copy(acc.at[3, own, part], out_ref.at[part], osem.at[h])
        o.start()
        outs.append(o)
    for s in range(15):
        kind, i = ("xi", s) if s < 2 else ("dm", s - 2) if s < 6 else ("xm", s - 6) if s < 14 else ("do", 0)
        there(kind, i).wait_send()
    for k in range(4):
        for i in range(3):
            send_x(k, i, own, 0).wait_send()
            send_y(k, i, own, 0).wait_send()
    for k in range(3):
        for h in range(2):
            send_z(k, h).wait_send()

    @pl.when(end)
    def _():
        for n in range(3):
            for q in range(4):
                inward(0, n, q).wait_send()

    @pl.when(jnp.logical_not(end))
    def _():
        for q in range(4):
            for n in range(2):
                across(0, n, q, inner).wait_send()
            remote(acc.at[0, order[q], line], ri.at[0, q], ms.at[2, q], mr.at[0, q], outer).wait_send()

    for o in outs:
        o.wait()


def reduce_gradients(x_in, dy_mid, x_mid, dy_out):
    bf, f32 = jnp.bfloat16, jnp.float32
    rows = 2 * x_in.shape[0]
    dma = pltpu.SemaphoreType.DMA
    any_spec = pl.BlockSpec(memory_space=pl.ANY)
    return pl.pallas_call(
        reduce_kernel,
        out_shape=jax.ShapeDtypeStruct((512, 512), f32),
        in_specs=[any_spec] * 4,
        out_specs=any_spec,
        scratch_shapes=[
            pltpu.VMEM((2, rows, 512), bf), pltpu.VMEM((4, rows, 512), bf), pltpu.VMEM((8, rows, 512), bf), pltpu.VMEM((rows, 512), bf),
            pltpu.VMEM((4, 4, 512, 512), f32), pltpu.VMEM((3, 3, PLANE, 512), f32), pltpu.VMEM((3, 3, PLANE, 512), f32),
            pltpu.VMEM((3, 256, 512), f32), pltpu.VMEM((3, 256, 512), f32), pltpu.VMEM((4, 2, PLANE, 512), f32),
            pltpu.VMEM((3, 4, LINE, 512), f32), pltpu.VMEM((2, 4, LINE, 512), f32),
            dma((15,)), dma((15,)), dma((15,)), dma((4, 3)), dma((4, 3)), dma((4, 3)), dma((4, 3)), dma((3, 2)), dma((4, 2)),
            dma((3, 4)), dma((3, 4)), dma((3, 4)), dma((2, 4)), dma((2,)),
        ],
        compiler_params=pltpu.CompilerParams(collective_id=0, has_side_effects=True, vmem_limit_bytes=67043328),
        name="reduce",
    )(x_in, dy_mid, x_mid, dy_out)


def gather_kernel(grad_in, rl_in, rr_in, sq_in, mom_in, sl_in, sr_in, w1_in, w2_in, new_left, new_right, new_sq, new_mom, w,
                  buf, grad, rl, rr, pre, isem, zs, zr, xs, xr, ys, yr, xds, xdr, yds, ydr, cs, cr):
    z, y, x, c = coords()
    xp, yp, cp = dev(z, y, 1 - x, c), dev(z, 1 - y, x, c), dev(z, y, x, 1 - c)

    def blk(zb, yb, xb, cb):
        return dev(zb, yb, xb, cb)[0]

    pairs = [(grad_in, grad), (rl_in, rl), (rr_in, rr), (sq_in, new_sq), (mom_in, new_mom), (sl_in, new_left), (sr_in, new_right), (w2_in, w.at[pl.ds(4096, 4096)])]
    pairs += [(w1_in.at[:, pl.ds(1024 * n, 1024)], w.at[pl.ds(1024 * n, 1024)]) for n in range(4)]
    loads = [pltpu.make_async_copy(src, dst, isem.at[i]) for i, (src, dst) in enumerate(pairs)]
    for load in loads[:5]:
        load.start()
    greet_signal(z, y, x, c)

    b0 = blk(z, y, x, c)
    for load in loads[:4]:
        load.wait()
    for load in loads[5:]:
        load.start()
    pre[...] = mm(rl[...], grad[...])
    rl[...] = mm(pre[...], rr[...])

    def strip_of(i):
        return pl.ds(pl.multiple_of(i * 64, 64), 64)

    def norms(i, sums):
        r = strip_of(i)
        g, p = grad[r], rl[r]
        sq = STAT_DECAY * new_sq[r] + (1.0 - STAT_DECAY) * g * g
        new_sq[r] = sq
        h = g / (jnp.sqrt(sq / BIAS_CORR) + GRAFT_EPS)
        return sums[0] + jnp.sum(h * h), sums[1] + jnp.sum(p * p)

    graft_sum, pre_sum = lax.fori_loop(0, 8, norms, (jnp.float32(0.0), jnp.float32(0.0)))
    loads[4].wait()
    ones = jnp.ones((64, 512), jnp.float32)
    scale = jnp.sqrt(graft_sum * ones) / jnp.sqrt(pre_sum * ones)

    def momentum_step(i, _):
        r = strip_of(i)
        mom = MOM_DECAY * new_mom[r] + rl[r] * scale
        new_mom[r] = mom
        buf[b0, r] = mom.astype(jnp.bfloat16)
        return 0

    lax.fori_loop(0, 8, momentum_step, 0)
    greet_wait()

    zb = [(z + 4 - h) % 4 for h in GATHER_HOPS]
    spots = [(y, x), (1 - y, x), (y, 1 - x), (1 - y, 1 - x)]

    def step(w, b, row, col):
        def strip(i, _):
            r = pl.ds(pl.multiple_of(row * 512 + i * 64, 64), 64)
            cc = pl.ds(pl.multiple_of(col * 512, 512), 512)
            old = w[r, cc]
            d = buf[b, pl.ds(pl.multiple_of(i * 64, 64), 64), :].astype(jnp.float32)
            w[r, cc] = old - LEARN_RATE * (d + WEIGHT_DECAY * old)
            return 0

        lax.fori_loop(0, 8, strip, 0)

    def apply(b, zk):
        first = zk < 2
        col = jnp.where(first, b % 8, b % 2)
        step(w, b, jnp.where(first, (col // 2) * 2 + b // 8, 8 + (b - 16) // 2), col % 2)

    def part(ref, b, h):
        return ref.at[b, pl.ds(h * 256, 256)]

    def xcopy(k, b):
        return remote(buf.at[b], buf.at[b], xs.at[k], xr.at[k], xp)

    def ycopy(k, b):
        return remote(buf.at[b], buf.at[b], ys.at[k], yr.at[k], yp)

    def xdiag(k, b):
        return remote(part(buf, b, 0), part(buf, b, 0), xds.at[k], xdr.at[k], xp)

    def ydiag(k, b):
        return remote(part(buf, b, 1), part(buf, b, 1), yds.at[k], ydr.at[k], yp)

    def ccopy(k, i, b):
        return remote(buf.at[b], buf.at[b], cs.at[k, i], cr.at[k, i], cp)

    def zcopy(k, b, peer):
        return remote(buf.at[b], buf.at[b], zs.at[k - 1], zr.at[k - 1], peer)

    xcopy(0, b0).start()
    ycopy(0, b0).start()
    for k in (1, 2, 3):
        zcopy(k, b0, dev((z + GATHER_HOPS[k]) % 4, y, x, c)).start()
    ccopy(0, 0, b0).start()
    for load in loads[5:7]:
        load.wait()
    pre[...] = mm(grad[...], grad[...], ((1,), (1,)))
    rr[...] = mm(grad[...], grad[...], ((0,), (0,)))

    def stats(i, _):
        r = strip_of(i)
        new_left[r] = STAT_DECAY * new_left[r] + (1.0 - STAT_DECAY) * pre[r]
        new_right[r] = STAT_DECAY * new_right[r] + (1.0 - STAT_DECAY) * rr[r]
        return 0

    lax.fori_loop(0, 8, stats, 0)
    for load in loads[7:]:
        load.wait()
    for k in range(4):
        b, by, bx, bd = [blk(zb[k], yy, xx, c) for yy, xx in spots]
        others = [blk(zb[k], yy, xx, 1 - c) for yy, xx in spots]
        ycopy(k, by).wait_recv()
        xdiag(k, by).start()
        ccopy(k, 1, by).start()
        xcopy(k, bx).wait_recv()
        ydiag(k, bx).start()
        ccopy(k, 2, bx).start()
        if k < 3:
            nb = blk(zb[k + 1], y, x, c)
            zcopy(k + 1, nb, xp).wait_recv()
            xcopy(k + 1, nb).start()
            ycopy(k + 1, nb).start()
            ccopy(k + 1, 0, nb).start()
        for t in (b, by, bx):
            apply(t, zb[k])
        for i in range(3):
            ccopy(k, i, others[i]).wait_recv()
            apply(others[i], zb[k])
        xdiag(k, bd).wait_recv()
        ydiag(k, bd).wait_recv()
        ccopy(k, 3, bd).start()
        apply(bd, zb[k])
        ccopy(k, 3, others[3]).wait_recv()
        apply(others[3], zb[k])
    for k in range(4):
        xcopy(k, b0).wait_send()
        ycopy(k, b0).wait_send()
        xdiag(k, b0).wait_send()
        ydiag(k, b0).wait_send()
        for i in range(4):
            ccopy(k, i, b0).wait_send()
        if k:
            zcopy(k, b0, xp).wait_send()


def finish_step(grad, root_left, root_right, graft_sq, momentum, stat_left, stat_right, w_fc1, w_fc2):
    bf, f32 = jnp.bfloat16, jnp.float32
    dma = pltpu.SemaphoreType.DMA
    any_spec = pl.BlockSpec(memory_space=pl.ANY)
    vmem_spec = pl.BlockSpec(memory_space=pltpu.VMEM)
    tile = pltpu.VMEM((512, 512), f32)
    return pl.pallas_call(
        gather_kernel,
        out_shape=(tile, tile, tile, tile, pltpu.VMEM((8192, 1024), f32)),
        in_specs=[any_spec] * 9,
        out_specs=(vmem_spec,) * 5,
        scratch_shapes=[pltpu.VMEM((32, 512, 512), bf)] + [pltpu.VMEM((512, 512), f32)] * 4 + [dma((12,)), dma((3,)), dma((3,))] + [dma((4,))] * 8 + [dma((4, 4)), dma((4, 4))],
        compiler_params=pltpu.CompilerParams(collective_id=1, has_side_effects=True, vmem_limit_bytes=26 * 2 ** 20),
        name="gather",
    )(grad, root_left, root_right, graft_sq, momentum, stat_left, stat_right, w_fc1, w_fc2)


def flush_kernel(left, right, sq, mom, w, left_out, right_out, sq_out, mom_out, w1_out, w2_out, sem):
    pairs = [(w.at[pl.ds(1024 * n, 1024)], w1_out.at[:, pl.ds(1024 * n, 1024)]) for n in range(4)]
    pairs += [(w.at[pl.ds(4096, 4096)], w2_out), (left, left_out), (right, right_out), (sq, sq_out), (mom, mom_out)]
    out = [pltpu.make_async_copy(src, dst, sem.at[i]) for i, (src, dst) in enumerate(pairs)]
    for o in out:
        o.start()
    for o in out:
        o.wait()


def flush(left, right, sq, mom, w, shape1, shape2):
    any_spec = pl.BlockSpec(memory_space=pl.ANY)
    tile = jax.ShapeDtypeStruct(left.shape, left.dtype)
    values = [pltpu.with_memory_space_constraint(v, pltpu.VMEM) for v in (left, right, sq, mom, w)]
    return pl.pallas_call(
        flush_kernel,
        out_shape=(tile, tile, tile, tile, jax.ShapeDtypeStruct(shape1, w.dtype), jax.ShapeDtypeStruct(shape2, w.dtype)),
        in_specs=[pl.BlockSpec(memory_space=pltpu.VMEM)] * 5,
        out_specs=(any_spec,) * 6,
        scratch_shapes=[pltpu.SemaphoreType.DMA((9,))],
        compiler_params=pltpu.CompilerParams(vmem_limit_bytes=2 ** 20),
        name="flush",
    )(*values)


def mm(a, b, dims=((1,), (0,))):
    return lax.dot_general(a, b, (dims, ((), ())), precision=lax.Precision.HIGHEST, preferred_element_type=jnp.float32)


def solution(mesh):
    def per_device(x_in, dy_mid, x_mid, dy_out, w_fc1, w_fc2, stat_left, stat_right, root_left, root_right, graft_sq, momentum):
        grad = reduce_gradients(x_in, dy_mid, x_mid, dy_out)
        done = finish_step(grad, root_left[0], root_right[0], graft_sq[0], momentum[0], stat_left[0], stat_right[0], w_fc1, w_fc2)
        new_left, new_right, new_sq, new_mom, new_w1, new_w2 = flush(*done, w_fc1.shape, w_fc2.shape)
        return new_w1, new_w2, new_left[None], new_right[None], new_sq[None], new_mom[None]

    row_spec = P('dp', None)
    rep_spec = P(None, None)
    tile_spec = P('dp', None, None)
    in_specs = (row_spec, row_spec, row_spec, row_spec, rep_spec, rep_spec, tile_spec, tile_spec, tile_spec, tile_spec, tile_spec, tile_spec)
    out_specs = (rep_spec, rep_spec, tile_spec, tile_spec, tile_spec, tile_spec)
    return jax.shard_map(per_device, mesh=mesh, in_specs=in_specs, out_specs=out_specs, check_vma=False)
```

```python
import functools

import jax
import jax.numpy as jnp
from jax import lax
from jax.experimental import pallas as pl
from jax.experimental.pallas import tpu as pltpu
from jax.sharding import PartitionSpec as P

STEP = 10
STAT_DECAY = 0.999
MOM_DECAY = 0.9
GRAFT_EPS = 1e-8
LEARN_RATE = 0.01
WEIGHT_DECAY = 1e-4
BIAS_CORR = 1.0 - STAT_DECAY ** STEP

MESH = pl.DeviceIdType.MESH
HOPS = (3, 2, 1, 0)
PLANE = 208
LINE = 512 - 2 * PLANE


def dev(z, y, x, c):
    return (((z * 2 + y) * 2 + x) * 2 + c,)


def coords():
    me = lax.axis_index("dp")
    return me // 8, (me // 4) % 2, (me // 2) % 2, me % 2


def greet_signal(z, y, x, c):
    peers = [dev(z, y, 1 - x, c), dev(z, 1 - y, x, c), dev(z, y, x, 1 - c)]
    peers += [dev((z + k) % 4, y, x, c) for k in (1, 2, 3)]
    for peer in peers:
        pl.semaphore_signal(pltpu.get_barrier_semaphore(), inc=1, device_id=peer, device_id_type=MESH)


def greet_wait():
    pl.semaphore_wait(pltpu.get_barrier_semaphore(), 6)


def remote(src, dst, send_sem, recv_sem, peer):
    return pltpu.make_async_remote_copy(src_ref=src, dst_ref=dst, send_sem=send_sem, recv_sem=recv_sem, device_id=peer, device_id_type=MESH)


def reduce_kernel(x_in, dy_mid, x_mid, dy_out, out_ref, xi, dm, xm, do, acc, rx, ry, rx3, ry3, rz, ro, ri, lsem, psem, qsem, xs, xr, ys, yr, zs, zr, ls, lr, ms, mr, osem):
    z, y, x, c = coords()
    rows = x_in.shape[0]
    bd = 512
    half = bd // 2
    xp, yp, cp = dev(z, y, 1 - x, c), dev(z, 1 - y, x, c), dev(z, y, x, 1 - c)
    own = y * 2 + x

    def cols(i):
        return pl.ds(pl.multiple_of(i * bd, bd), bd)

    def operand(kind, i):
        if kind == "xi":
            return i, x_in.at[:, cols(i)], x_in.at[:, cols(i)], xi.at[i]
        if kind == "dm":
            return 2 + i, dy_mid.at[:, cols(2 * i + c)], dy_mid.at[:, cols(2 * i + 1 - c)], dm.at[i]
        if kind == "xm":
            return 6 + i, x_mid.at[:, cols(i)], x_mid.at[:, cols(i)], xm.at[i]
        return 14, dy_out.at[:, cols(c)], dy_out.at[:, cols(1 - c)], do

    def here(kind, i):
        s, mine, _, dst = operand(kind, i)
        return pltpu.make_async_copy(mine, dst.at[pl.ds(0, rows)], lsem.at[s])

    def there(kind, i):
        s, _, theirs, dst = operand(kind, i)
        return remote(theirs, dst.at[pl.ds(rows, rows)], qsem.at[s], psem.at[s], cp)

    def fetch(kind, i):
        there(kind, i).start()
        here(kind, i).start()

    def arrive(kind, i):
        here(kind, i).wait()
        there(kind, i).wait_recv()

    greet_signal(z, y, x, c)
    greet_wait()

    low = z < 2
    end = (z == 0) | (z == 3)
    hop = [jnp.where(low, h, (4 - h) % 4) for h in HOPS]
    zb = [(z + h) % 4 for h in hop]
    inner = dev(jnp.where(low, z + 1, z - 1), y, x, c)
    outer = dev(jnp.where(low, 0, 3), y, x, c)
    far = dev(jnp.where(low, 3, 0), y, x, c)
    first1 = [zb[0] < 2, (zb[1] < 2) & (zb[0] >= 2)]
    first2 = [zb[0] >= 2, (zb[1] >= 2) & (zb[0] < 2)]
    first1 += [(zb[2] < 2) & (zb[0] >= 2) & (zb[1] >= 2), zb[0] < 0]
    first2 += [(zb[2] >= 2) & (zb[0] < 2) & (zb[1] < 2), zb[0] < 0]
    order = [(1 - y) * 2 + 1 - x, y * 2 + 1 - x, (1 - y) * 2 + x, own]

    for k in range(4):
        @pl.when(zb[k] < 2)
        def _():
            fetch("xi", zb[k])

        @pl.when(first2[k])
        def _():
            fetch("do", 0)

        for q in range(4):
            @pl.when(first1[k])
            def _():
                fetch("dm", order[q])

            @pl.when(zb[k] >= 2)
            def _():
                fetch("xm", (zb[k] - 2) * 4 + order[q])

    def dots(lhs, rhs, dst):
        for h in range(2):
            dst[h * half:(h + 1) * half] = lax.dot_general(lhs[:, h * half:(h + 1) * half], rhs[...], (((0,), (0,)), ((), ())), preferred_element_type=jnp.float32)

    def size(k):
        return half if k == 3 else PLANE

    def rows_of(k, h):
        return pl.ds(h * size(k), size(k))

    def slot_x(k, i):
        return rx3.at[i] if k == 3 else rx.at[k, i]

    def slot_y(k, i):
        return ry3.at[i] if k == 3 else ry.at[k, i]

    def send_x(k, i, j, h):
        return remote(acc.at[k, j, rows_of(k, h)], slot_x(k, i), xs.at[k, i], xr.at[k, i], xp)

    def send_y(k, i, j, h):
        return remote(acc.at[k, j, rows_of(k, h)], slot_y(k, i), ys.at[k, i], yr.at[k, i], yp)

    def send_one(q, j):
        @pl.when(q < 2)
        def _():
            remote(acc.at[0, j, rows_of(0, 0)], rx.at[0, q], xs.at[0, q], xr.at[0, q], xp).start()

        @pl.when(q % 2 == 0)
        def _():
            remote(acc.at[0, j, rows_of(0, 1)], ry.at[0, q // 2], ys.at[0, q // 2], yr.at[0, q // 2], yp).start()

    line = pl.ds(2 * PLANE, LINE)

    def inward(k, n, q):
        return remote(acc.at[k, order_of(q), line], ro.at[n, q], ls.at[n, q], lr.at[n, q], inner)

    def across(k, n, q, peer):
        return remote(acc.at[k, order_of(q), line], ri.at[n, q], ms.at[n, q], mr.at[n, q], peer)

    def order_of(q):
        return order[q] if isinstance(q, int) else pick(order, q)

    def pass_on(n, q):
        inward(0, n, q).wait_recv()
        acc[n + 1, order_of(q), line] += ro[n, q]
        across(n + 1, n, q, inner).start()

    def pick(values, i):
        out = values[-1]
        for n in range(len(values) - 2, -1, -1):
            out = jnp.where(i == n, values[n], out)
        return out

    def group(k, _):
        zk = pick(zb, k)
        f1, f2 = pick([v.astype(jnp.int32) for v in first1], k), pick([v.astype(jnp.int32) for v in first2], k)

        @pl.when(zk < 2)
        def _():
            arrive("xi", zk)

        @pl.when(f2 == 1)
        def _():
            arrive("do", 0)

        def tile(q, _):
            j = pick(order, q)

            @pl.when(f1 == 1)
            def _():
                arrive("dm", j)

            @pl.when(zk < 2)
            def _():
                dots(xi.at[zk], dm.at[j], acc.at[k, j])

            @pl.when(zk >= 2)
            def _():
                t = (zk - 2) * 4 + j
                arrive("xm", t)
                dots(xm.at[t], do, acc.at[k, j])

            @pl.when(k < 1)
            def _():
                send_one(q, j)

            @pl.when(end & (k < 3))
            def _():
                inward(k, k, q).start()

            @pl.when(jnp.logical_not(end) & (k == 2))
            def _():
                pass_on(0, q)

            return 0

        return lax.fori_loop(0, 4, tile, 0)

    lax.fori_loop(0, 2, group, 0)

    def add(k, j, where, ref):
        acc[k, j, where] += ref[...]

    def start_one(k):
        send_x(k, 0, order[0], 0).start()
        send_y(k, 0, order[0], 1).start()
        send_x(k, 1, order[1], 0).start()
        send_y(k, 1, order[2], 1).start()

    def start_two(k):
        send_x(k, 0, own, 0).wait_recv()
        add(k, order[2], rows_of(k, 0), slot_x(k, 0))
        send_y(k, 2, order[2], 0).start()
        send_y(k, 0, own, 1).wait_recv()
        add(k, order[1], rows_of(k, 1), slot_y(k, 0))
        send_x(k, 2, order[1], 1).start()

    def send_z(k, h):
        n = jnp.where(end, k, (0, 1, 3)[k])
        peer = (jnp.where(end, inner[0], (outer, far, inner)[k][0]),)
        return remote(acc.at[k, own, rows_of(k, h)], rz.at[n, h], zs.at[k, h], zr.at[n, h], peer)

    def got_z(n, h):
        remote(rz.at[n, h], rz.at[n, h], zs.at[0, h], zr.at[n, h], inner).wait_recv()

    def relay(k):
        @pl.when(jnp.logical_not(end))
        def _():
            for h in range(2):
                got_z(k - 1, h)
                add(k, own, rows_of(k, h), rz.at[k - 1, h])
                send_z(k, h).start()

    def leave(k, h):
        if k == 0:
            send_z(k, h).start()
        elif k < 3:
            @pl.when(end)
            def _():
                send_z(k, h).start()

    def finish_plane(k):
        send_x(k, 1, own, 0).wait_recv()
        add(k, own, rows_of(k, 0), slot_x(k, 1))
        send_y(k, 1, own, 1).wait_recv()
        add(k, own, rows_of(k, 1), slot_y(k, 1))
        send_y(k, 2, own, 0).wait_recv()
        add(k, own, rows_of(k, 0), slot_y(k, 2))
        leave(k, 0)
        send_x(k, 2, own, 1).wait_recv()
        add(k, own, rows_of(k, 1), slot_x(k, 2))
        leave(k, 1)

    def line_first(n):
        @pl.when(jnp.logical_not(end))
        def _():
            for q in range(4):
                pass_on(n, q)

    def line_second():
        @pl.when(jnp.logical_not(end))
        def _():
            for q in range(4):
                across(0, 0, q, inner).wait_recv()
                add(0, order[q], line, ri.at[0, q])
                remote(acc.at[0, order[q], line], ri.at[0, q], ms.at[2, q], mr.at[0, q], outer).start()

    def line_last():
        @pl.when(end)
        def _():
            for q in range(4):
                across(0, 0, q, inner).wait_recv()
                add(3, order[q], line, ri.at[0, q])

        @pl.when(jnp.logical_not(end))
        def _():
            for q in range(4):
                inward(0, 2, q).wait_recv()
                add(3, order[q], line, ro.at[2, q])
                across(0, 1, q, inner).wait_recv()
                add(3, order[q], line, ri.at[1, q])

    start_two(0)
    start_one(1)
    lax.fori_loop(2, 4, group, 0)
    finish_plane(0)
    start_two(1)
    start_one(2)
    line_first(1)
    line_second()
    finish_plane(1)
    start_two(2)
    line_last()
    start_one(3)
    relay(1)
    finish_plane(2)
    start_two(3)
    relay(2)
    finish_plane(3)

    for n in range(2):
        for h in range(2):
            slot = jnp.where(end, n, n + 2)
            got_z(slot, h)
            add(3, own, rows_of(0, h), rz.at[slot, h])
    outs = []
    for h in range(2):
        part = pl.ds(h * half, half)
        acc[3, own, part] = acc[3, own, part] * (1.0 / 32.0)
        o = pltpu.make_async_copy(acc.at[3, own, part], out_ref.at[part], osem.at[h])
        o.start()
        outs.append(o)
    for s in range(15):
        kind, i = ("xi", s) if s < 2 else ("dm", s - 2) if s < 6 else ("xm", s - 6) if s < 14 else ("do", 0)
        there(kind, i).wait_send()
    for k in range(4):
        for i in range(3):
            send_x(k, i, own, 0).wait_send()
            send_y(k, i, own, 0).wait_send()
    for k in range(3):
        for h in range(2):
            send_z(k, h).wait_send()

    @pl.when(end)
    def _():
        for n in range(3):
            for q in range(4):
                inward(0, n, q).wait_send()

    @pl.when(jnp.logical_not(end))
    def _():
        for q in range(4):
            for n in range(2):
                across(0, n, q, inner).wait_send()
            remote(acc.at[0, order[q], line], ri.at[0, q], ms.at[2, q], mr.at[0, q], outer).wait_send()

    for o in outs:
        o.wait()


def reduce_gradients(x_in, dy_mid, x_mid, dy_out):
    bf, f32 = jnp.bfloat16, jnp.float32
    rows = 2 * x_in.shape[0]
    dma = pltpu.SemaphoreType.DMA
    any_spec = pl.BlockSpec(memory_space=pl.ANY)
    return pl.pallas_call(
        reduce_kernel,
        out_shape=jax.ShapeDtypeStruct((512, 512), f32),
        in_specs=[any_spec] * 4,
        out_specs=any_spec,
        scratch_shapes=[
            pltpu.VMEM((2, rows, 512), bf), pltpu.VMEM((4, rows, 512), bf), pltpu.VMEM((8, rows, 512), bf), pltpu.VMEM((rows, 512), bf),
            pltpu.VMEM((4, 4, 512, 512), f32), pltpu.VMEM((3, 3, PLANE, 512), f32), pltpu.VMEM((3, 3, PLANE, 512), f32),
            pltpu.VMEM((3, 256, 512), f32), pltpu.VMEM((3, 256, 512), f32), pltpu.VMEM((4, 2, PLANE, 512), f32),
            pltpu.VMEM((3, 4, LINE, 512), f32), pltpu.VMEM((2, 4, LINE, 512), f32),
            dma((15,)), dma((15,)), dma((15,)), dma((4, 3)), dma((4, 3)), dma((4, 3)), dma((4, 3)), dma((3, 2)), dma((4, 2)),
            dma((3, 4)), dma((3, 4)), dma((3, 4)), dma((2, 4)), dma((2,)),
        ],
        compiler_params=pltpu.CompilerParams(collective_id=0, has_side_effects=True, vmem_limit_bytes=67043328),
        name="reduce",
    )(x_in, dy_mid, x_mid, dy_out)


def gather_kernel(grad_in, rl_in, rr_in, sq_in, mom_in, sl_in, sr_in, w1_in, w2_in, new_left, new_right, new_sq, new_mom, w,
                  buf, grad, rl, rr, pre, isem, zs, zr, xs, xr, ys, yr, xds, xdr, yds, ydr, cs, cr, ls, lr, lcs, lcr):
    z, y, x, c = coords()
    xp, yp, cp = dev(z, y, 1 - x, c), dev(z, 1 - y, x, c), dev(z, y, x, 1 - c)

    pairs = [(grad_in, grad), (rl_in, rl), (rr_in, rr), (sq_in, new_sq), (mom_in, new_mom), (sl_in, new_left), (sr_in, new_right), (w2_in, w.at[pl.ds(4096, 4096)])]
    pairs += [(w1_in.at[:, pl.ds(1024 * n, 1024)], w.at[pl.ds(1024 * n, 1024)]) for n in range(4)]
    loads = [pltpu.make_async_copy(src, dst, isem.at[i]) for i, (src, dst) in enumerate(pairs)]
    for load in loads[:5]:
        load.start()
    greet_signal(z, y, x, c)

    own = y * 2 + x
    for load in loads[:4]:
        load.wait()
    for load in loads[5:]:
        load.start()
    pre[...] = mm(rl[...], grad[...])
    rl[...] = mm(pre[...], rr[...])

    def strip_of(i):
        return pl.ds(pl.multiple_of(i * 64, 64), 64)

    def norms(i, sums):
        r = strip_of(i)
        g, p = grad[r], rl[r]
        sq = STAT_DECAY * new_sq[r] + (1.0 - STAT_DECAY) * g * g
        new_sq[r] = sq
        h = g / (jnp.sqrt(sq / BIAS_CORR) + GRAFT_EPS)
        return sums[0] + jnp.sum(h * h), sums[1] + jnp.sum(p * p)

    graft_sum, pre_sum = lax.fori_loop(0, 8, norms, (jnp.float32(0.0), jnp.float32(0.0)))
    loads[4].wait()
    ones = jnp.ones((64, 512), jnp.float32)
    scale = jnp.sqrt(graft_sum * ones) / jnp.sqrt(pre_sum * ones)

    def momentum_step(i, _):
        r = strip_of(i)
        mom = MOM_DECAY * new_mom[r] + rl[r] * scale
        new_mom[r] = mom
        buf[z, own, c, r] = mom.astype(jnp.bfloat16)
        return 0

    lax.fori_loop(0, 8, momentum_step, 0)
    greet_wait()

    low = z < 2
    end = (z == 0) | (z == 3)
    middle = jnp.logical_not(end)
    near = [jnp.where(end, n, m) for n, m in ((1, 0), (2, 2), (3, 3))]
    zb = [z] + [jnp.where(low, n, 3 - n) for n in near]
    inner = dev(jnp.where(low, z + 1, z - 1), y, x, c)
    outer = dev(jnp.where(low, 0, 3), y, x, c)
    yx = [own, (1 - y) * 2 + x, y * 2 + 1 - x, (1 - y) * 2 + 1 - x]
    line = pl.ds(2 * PLANE, LINE)

    def step(zk, n, cb, first, count):
        b = (zk * 4 + n) * 2 + cb
        upper = zk < 2
        col = jnp.where(upper, b % 8, b % 2)
        row = jnp.where(upper, (col // 2) * 2 + b // 8, 8 + (b - 16) // 2)

        def strip(i, _):
            at = first + i * 32
            r = pl.ds(pl.multiple_of(row * 512 + at, 32), 32)
            cc = pl.ds(pl.multiple_of((col % 2) * 512, 512), 512)
            old = w[r, cc]
            d = buf[zk, n, cb, pl.ds(pl.multiple_of(at, 32), 32), :].astype(jnp.float32)
            w[r, cc] = old - LEARN_RATE * (d + WEIGHT_DECAY * old)
            return 0

        lax.fori_loop(0, count, strip, 0)

    def plane_rows(k):
        return 512 if k == 0 else 2 * PLANE

    def same(zk, n, where, ss, rs, peer):
        ref = buf.at[zk, n, c, where]
        return remote(ref, ref, ss, rs, peer)

    def xcopy(k, n):
        return same(zb[k], n, pl.ds(0, plane_rows(k)), xs.at[k], xr.at[k], xp)

    def ycopy(k, n):
        return same(zb[k], n, pl.ds(0, plane_rows(k)), ys.at[k], yr.at[k], yp)

    def xdiag(k, n):
        return same(zb[k], n, pl.ds(0, plane_rows(k) // 2), xds.at[k], xdr.at[k], xp)

    def ydiag(k, n):
        return same(zb[k], n, pl.ds(plane_rows(k) // 2, plane_rows(k) // 2), yds.at[k], ydr.at[k], yp)

    def ccopy(k, i, n):
        return same(zb[k], n, pl.ds(0, plane_rows(k)), cs.at[k, i], cr.at[k, i], cp)

    def zcopy(layer, n, peer):
        return same(layer, own, pl.ds(0, 2 * PLANE), zs.at[n], zr.at[layer], peer)

    def zpass(k):
        return zcopy(zb[k], k + 1, inner if k == 1 else outer)

    def zown():
        return zcopy(z, 0, inner), zcopy(z, 1, outer)

    def lines(layer, ss, rs, peer):
        ref = buf.at[layer, :, c, line]
        return remote(ref, ref, ss, rs, peer)

    def forward(k):
        return lines(zb[k], ls.at[k + 1], lr.at[zb[k]], inner if k == 1 else outer)

    def line_core(k):
        return lines(zb[k], lcs.at[k - 1], lcr.at[k - 1], cp)

    def start_line():
        lines(z, ls.at[0], lr.at[z], inner).start()

        @pl.when(middle)
        def _():
            lines(z, ls.at[1], lr.at[z], outer).start()

    def take_line(k, where):
        @pl.when(where)
        def _():
            forward(k).wait_recv()
            if where is middle:
                forward(k).start()
            line_core(k).start()

    def apply_line(k):
        line_core(k).wait_recv()
        for n in range(4):
            for cb in range(2):
                step(zb[k], n, cb, 2 * PLANE, LINE // 32)

    xcopy(0, own).start()
    ycopy(0, own).start()
    to_inner, to_outer = zown()
    to_inner.start()

    @pl.when(middle)
    def _():
        to_outer.start()

    ccopy(0, 0, own).start()
    for load in loads[5:7]:
        load.wait()
    pre[...] = mm(grad[...], grad[...], ((1,), (1,)))
    rr[...] = mm(grad[...], grad[...], ((0,), (0,)))

    def stats(i, _):
        r = strip_of(i)
        new_left[r] = STAT_DECAY * new_left[r] + (1.0 - STAT_DECAY) * pre[r]
        new_right[r] = STAT_DECAY * new_right[r] + (1.0 - STAT_DECAY) * rr[r]
        return 0

    lax.fori_loop(0, 8, stats, 0)
    for load in loads[7:]:
        load.wait()

    def meet(k):
        ycopy(k, yx[1]).wait_recv()
        xdiag(k, yx[1]).start()
        ccopy(k, 1, yx[1]).start()
        xcopy(k, yx[2]).wait_recv()
        ydiag(k, yx[2]).start()
        ccopy(k, 2, yx[2]).start()

    def begin(k):
        xcopy(k, own).start()
        ycopy(k, own).start()
        ccopy(k, 0, own).start()

    def use(k):
        for i in range(3):
            step(zb[k], yx[i], c, 0, plane_rows(k) // 32)
        for i in range(3):
            ccopy(k, i, yx[i]).wait_recv()
            step(zb[k], yx[i], 1 - c, 0, plane_rows(k) // 32)

    def meet_last(k):
        xdiag(k, yx[3]).wait_recv()
        ydiag(k, yx[3]).wait_recv()
        ccopy(k, 3, yx[3]).start()

    def use_last(k):
        step(zb[k], yx[3], c, 0, plane_rows(k) // 32)
        ccopy(k, 3, yx[3]).wait_recv()
        step(zb[k], yx[3], 1 - c, 0, plane_rows(k) // 32)

    def pass_z(k):
        zpass(k).wait_recv()
        zpass(k).start()

    meet(0)

    @pl.when(end)
    def _():
        zpass(1).wait_recv()

    @pl.when(middle)
    def _():
        pass_z(1)
        pass_z(2)

    begin(1)
    use(0)
    meet_last(0)
    start_line()

    @pl.when(end)
    def _():
        zpass(2).wait_recv()

    @pl.when(middle)
    def _():
        pass_z(3)

    begin(2)
    use_last(0)
    meet(1)
    take_line(1, middle)

    @pl.when(end)
    def _():
        zpass(3).wait_recv()

    begin(3)
    take_line(2, middle)
    take_line(1, end)
    use(1)
    meet_last(1)
    meet(2)
    take_line(3, middle)
    use_last(1)
    apply_line(1)
    use(2)
    meet_last(2)
    take_line(2, end)
    use_last(2)
    apply_line(2)
    meet(3)
    use(3)
    take_line(3, end)
    apply_line(3)
    meet_last(3)
    use_last(3)

    for k in range(4):
        xcopy(k, own).wait_send()
        ycopy(k, own).wait_send()
        xdiag(k, own).wait_send()
        ydiag(k, own).wait_send()
        for i in range(4):
            ccopy(k, i, own).wait_send()
        if k:
            line_core(k).wait_send()
    to_inner.wait_send()
    lines(z, ls.at[0], lr.at[z], inner).wait_send()

    @pl.when(middle)
    def _():
        to_outer.wait_send()
        lines(z, ls.at[1], lr.at[z], outer).wait_send()
        for k in (1, 2, 3):
            zpass(k).wait_send()
            forward(k).wait_send()


def finish_step(grad, root_left, root_right, graft_sq, momentum, stat_left, stat_right, w_fc1, w_fc2):
    bf, f32 = jnp.bfloat16, jnp.float32
    dma = pltpu.SemaphoreType.DMA
    any_spec = pl.BlockSpec(memory_space=pl.ANY)
    vmem_spec = pl.BlockSpec(memory_space=pltpu.VMEM)
    tile = pltpu.VMEM((512, 512), f32)
    return pl.pallas_call(
        gather_kernel,
        out_shape=(tile, tile, tile, tile, pltpu.VMEM((8192, 1024), f32)),
        in_specs=[any_spec] * 9,
        out_specs=(vmem_spec,) * 5,
        scratch_shapes=[pltpu.VMEM((4, 4, 2, 512, 512), bf)] + [pltpu.VMEM((512, 512), f32)] * 4 + [dma((12,)), dma((5,)), dma((4,))] + [dma((4,))] * 8 + [dma((4, 4)), dma((4, 4)), dma((5,)), dma((4,)), dma((3,)), dma((3,))],
        compiler_params=pltpu.CompilerParams(collective_id=1, has_side_effects=True, vmem_limit_bytes=26 * 2 ** 20),
        name="gather",
    )(grad, root_left, root_right, graft_sq, momentum, stat_left, stat_right, w_fc1, w_fc2)


def flush_kernel(left, right, sq, mom, w, left_out, right_out, sq_out, mom_out, w1_out, w2_out, sem):
    pairs = [(w.at[pl.ds(1024 * n, 1024)], w1_out.at[:, pl.ds(1024 * n, 1024)]) for n in range(4)]
    pairs += [(w.at[pl.ds(4096, 4096)], w2_out), (left, left_out), (right, right_out), (sq, sq_out), (mom, mom_out)]
    out = [pltpu.make_async_copy(src, dst, sem.at[i]) for i, (src, dst) in enumerate(pairs)]
    for o in out:
        o.start()
    for o in out:
        o.wait()


def flush(left, right, sq, mom, w, shape1, shape2):
    any_spec = pl.BlockSpec(memory_space=pl.ANY)
    tile = jax.ShapeDtypeStruct(left.shape, left.dtype)
    values = [pltpu.with_memory_space_constraint(v, pltpu.VMEM) for v in (left, right, sq, mom, w)]
    return pl.pallas_call(
        flush_kernel,
        out_shape=(tile, tile, tile, tile, jax.ShapeDtypeStruct(shape1, w.dtype), jax.ShapeDtypeStruct(shape2, w.dtype)),
        in_specs=[pl.BlockSpec(memory_space=pltpu.VMEM)] * 5,
        out_specs=(any_spec,) * 6,
        scratch_shapes=[pltpu.SemaphoreType.DMA((9,))],
        compiler_params=pltpu.CompilerParams(vmem_limit_bytes=2 ** 20),
        name="flush",
    )(*values)


def mm(a, b, dims=((1,), (0,))):
    return lax.dot_general(a, b, (dims, ((), ())), precision=lax.Precision.HIGHEST, preferred_element_type=jnp.float32)


def solution(mesh):
    def per_device(x_in, dy_mid, x_mid, dy_out, w_fc1, w_fc2, stat_left, stat_right, root_left, root_right, graft_sq, momentum):
        grad = reduce_gradients(x_in, dy_mid, x_mid, dy_out)
        done = finish_step(grad, root_left[0], root_right[0], graft_sq[0], momentum[0], stat_left[0], stat_right[0], w_fc1, w_fc2)
        new_left, new_right, new_sq, new_mom, new_w1, new_w2 = flush(*done, w_fc1.shape, w_fc2.shape)
        return new_w1, new_w2, new_left[None], new_right[None], new_sq[None], new_mom[None]

    row_spec = P('dp', None)
    rep_spec = P(None, None)
    tile_spec = P('dp', None, None)
    in_specs = (row_spec, row_spec, row_spec, row_spec, rep_spec, rep_spec, tile_spec, tile_spec, tile_spec, tile_spec, tile_spec, tile_spec)
    out_specs = (rep_spec, rep_spec, tile_spec, tile_spec, tile_spec, tile_spec)
    return jax.shard_map(per_device, mesh=mesh, in_specs=in_specs, out_specs=out_specs, check_vma=False)
```

```python
import functools

import jax
import jax.numpy as jnp
from jax import lax
from jax.experimental import pallas as pl
from jax.experimental.pallas import tpu as pltpu
from jax.sharding import PartitionSpec as P

STEP = 10
STAT_DECAY = 0.999
MOM_DECAY = 0.9
GRAFT_EPS = 1e-8
LEARN_RATE = 0.01
WEIGHT_DECAY = 1e-4
BIAS_CORR = 1.0 - STAT_DECAY ** STEP

MESH = pl.DeviceIdType.MESH
HOPS = (3, 2, 1, 0)
PLANE = 208
LINE = 512 - 2 * PLANE
GATHER_PLANE = 208
GATHER_LINE = 512 - 2 * GATHER_PLANE


def dev(z, y, x, c):
    return (((z * 2 + y) * 2 + x) * 2 + c,)


def coords():
    me = lax.axis_index("dp")
    return me // 8, (me // 4) % 2, (me // 2) % 2, me % 2


def greet_signal(z, y, x, c):
    peers = [dev(z, y, 1 - x, c), dev(z, 1 - y, x, c), dev(z, y, x, 1 - c)]
    peers += [dev((z + k) % 4, y, x, c) for k in (1, 2, 3)]
    for peer in peers:
        pl.semaphore_signal(pltpu.get_barrier_semaphore(), inc=1, device_id=peer, device_id_type=MESH)


def greet_wait():
    pl.semaphore_wait(pltpu.get_barrier_semaphore(), 6)


def remote(src, dst, send_sem, recv_sem, peer):
    return pltpu.make_async_remote_copy(src_ref=src, dst_ref=dst, send_sem=send_sem, recv_sem=recv_sem, device_id=peer, device_id_type=MESH)


def reduce_kernel(x_in, dy_mid, x_mid, dy_out, out_ref, xi, dm, xm, do, acc, rx, ry, rx3, ry3, rz, ro, ri, lsem, psem, qsem, xs, xr, ys, yr, zs, zr, ls, lr, ms, mr, osem):
    z, y, x, c = coords()
    rows = x_in.shape[0]
    bd = 512
    half = bd // 2
    xp, yp, cp = dev(z, y, 1 - x, c), dev(z, 1 - y, x, c), dev(z, y, x, 1 - c)
    own = y * 2 + x

    def cols(i):
        return pl.ds(pl.multiple_of(i * bd, bd), bd)

    def operand(kind, i):
        if kind == "xi":
            return i, x_in.at[:, cols(i)], x_in.at[:, cols(i)], xi.at[i]
        if kind == "dm":
            return 2 + i, dy_mid.at[:, cols(2 * i + c)], dy_mid.at[:, cols(2 * i + 1 - c)], dm.at[i]
        if kind == "xm":
            return 6 + i, x_mid.at[:, cols(i)], x_mid.at[:, cols(i)], xm.at[i]
        return 14, dy_out.at[:, cols(c)], dy_out.at[:, cols(1 - c)], do

    def here(kind, i):
        s, mine, _, dst = operand(kind, i)
        return pltpu.make_async_copy(mine, dst.at[pl.ds(0, rows)], lsem.at[s])

    def there(kind, i):
        s, _, theirs, dst = operand(kind, i)
        return remote(theirs, dst.at[pl.ds(rows, rows)], qsem.at[s], psem.at[s], cp)

    def fetch(kind, i):
        there(kind, i).start()
        here(kind, i).start()

    def arrive(kind, i):
        here(kind, i).wait()
        there(kind, i).wait_recv()

    greet_signal(z, y, x, c)
    greet_wait()

    low = z < 2
    end = (z == 0) | (z == 3)
    hop = [jnp.where(low, h, (4 - h) % 4) for h in HOPS]
    zb = [(z + h) % 4 for h in hop]
    inner = dev(jnp.where(low, z + 1, z - 1), y, x, c)
    outer = dev(jnp.where(low, 0, 3), y, x, c)
    far = dev(jnp.where(low, 3, 0), y, x, c)
    first1 = [zb[0] < 2, (zb[1] < 2) & (zb[0] >= 2)]
    first2 = [zb[0] >= 2, (zb[1] >= 2) & (zb[0] < 2)]
    first1 += [(zb[2] < 2) & (zb[0] >= 2) & (zb[1] >= 2), zb[0] < 0]
    first2 += [(zb[2] >= 2) & (zb[0] < 2) & (zb[1] < 2), zb[0] < 0]
    order = [(1 - y) * 2 + 1 - x, y * 2 + 1 - x, (1 - y) * 2 + x, own]

    for k in range(4):
        @pl.when(zb[k] < 2)
        def _():
            fetch("xi", zb[k])

        @pl.when(first2[k])
        def _():
            fetch("do", 0)

        for q in range(4):
            @pl.when(first1[k])
            def _():
                fetch("dm", order[q])

            @pl.when(zb[k] >= 2)
            def _():
                fetch("xm", (zb[k] - 2) * 4 + order[q])

    def dots(lhs, rhs, dst):
        for h in range(2):
            dst[h * half:(h + 1) * half] = lax.dot_general(lhs[:, h * half:(h + 1) * half], rhs[...], (((0,), (0,)), ((), ())), preferred_element_type=jnp.float32)

    def size(k):
        return half if k == 3 else PLANE

    def rows_of(k, h):
        return pl.ds(h * size(k), size(k))

    def slot_x(k, i):
        return rx3.at[i] if k == 3 else rx.at[k, i]

    def slot_y(k, i):
        return ry3.at[i] if k == 3 else ry.at[k, i]

    def send_x(k, i, j, h):
        return remote(acc.at[k, j, rows_of(k, h)], slot_x(k, i), xs.at[k, i], xr.at[k, i], xp)

    def send_y(k, i, j, h):
        return remote(acc.at[k, j, rows_of(k, h)], slot_y(k, i), ys.at[k, i], yr.at[k, i], yp)

    def send_one(q, j):
        @pl.when(q < 2)
        def _():
            remote(acc.at[0, j, rows_of(0, 0)], rx.at[0, q], xs.at[0, q], xr.at[0, q], xp).start()

        @pl.when(q % 2 == 0)
        def _():
            remote(acc.at[0, j, rows_of(0, 1)], ry.at[0, q // 2], ys.at[0, q // 2], yr.at[0, q // 2], yp).start()

    line = pl.ds(2 * PLANE, LINE)

    def inward(k, n, q):
        return remote(acc.at[k, order_of(q), line], ro.at[n, q], ls.at[n, q], lr.at[n, q], inner)

    def across(k, n, q, peer):
        return remote(acc.at[k, order_of(q), line], ri.at[n, q], ms.at[n, q], mr.at[n, q], peer)

    def order_of(q):
        return order[q] if isinstance(q, int) else pick(order, q)

    def pass_on(n, q):
        inward(0, n, q).wait_recv()
        acc[n + 1, order_of(q), line] += ro[n, q]
        across(n + 1, n, q, inner).start()

    def pick(values, i):
        out = values[-1]
        for n in range(len(values) - 2, -1, -1):
            out = jnp.where(i == n, values[n], out)
        return out

    def group(k, _):
        zk = pick(zb, k)
        f1, f2 = pick([v.astype(jnp.int32) for v in first1], k), pick([v.astype(jnp.int32) for v in first2], k)

        @pl.when(zk < 2)
        def _():
            arrive("xi", zk)

        @pl.when(f2 == 1)
        def _():
            arrive("do", 0)

        def tile(q, _):
            j = pick(order, q)

            @pl.when(f1 == 1)
            def _():
                arrive("dm", j)

            @pl.when(zk < 2)
            def _():
                dots(xi.at[zk], dm.at[j], acc.at[k, j])

            @pl.when(zk >= 2)
            def _():
                t = (zk - 2) * 4 + j
                arrive("xm", t)
                dots(xm.at[t], do, acc.at[k, j])

            @pl.when(k < 1)
            def _():
                send_one(q, j)

            @pl.when(end & (k < 3))
            def _():
                inward(k, k, q).start()

            @pl.when(jnp.logical_not(end) & (k == 2))
            def _():
                pass_on(0, q)

            return 0

        return lax.fori_loop(0, 4, tile, 0)

    lax.fori_loop(0, 2, group, 0)

    def add(k, j, where, ref):
        acc[k, j, where] += ref[...]

    def start_one(k):
        send_x(k, 0, order[0], 0).start()
        send_y(k, 0, order[0], 1).start()
        send_x(k, 1, order[1], 0).start()
        send_y(k, 1, order[2], 1).start()

    def start_two(k):
        send_x(k, 0, own, 0).wait_recv()
        add(k, order[2], rows_of(k, 0), slot_x(k, 0))
        send_y(k, 2, order[2], 0).start()
        send_y(k, 0, own, 1).wait_recv()
        add(k, order[1], rows_of(k, 1), slot_y(k, 0))
        send_x(k, 2, order[1], 1).start()

    def send_z(k, h):
        n = jnp.where(end, k, (0, 1, 3)[k])
        peer = (jnp.where(end, inner[0], (outer, far, inner)[k][0]),)
        return remote(acc.at[k, own, rows_of(k, h)], rz.at[n, h], zs.at[k, h], zr.at[n, h], peer)

    def got_z(n, h):
        remote(rz.at[n, h], rz.at[n, h], zs.at[0, h], zr.at[n, h], inner).wait_recv()

    def relay(k):
        @pl.when(jnp.logical_not(end))
        def _():
            for h in range(2):
                got_z(k - 1, h)
                add(k, own, rows_of(k, h), rz.at[k - 1, h])
                send_z(k, h).start()

    def leave(k, h):
        if k == 0:
            send_z(k, h).start()
        elif k < 3:
            @pl.when(end)
            def _():
                send_z(k, h).start()

    def finish_plane(k):
        send_x(k, 1, own, 0).wait_recv()
        add(k, own, rows_of(k, 0), slot_x(k, 1))
        send_y(k, 1, own, 1).wait_recv()
        add(k, own, rows_of(k, 1), slot_y(k, 1))
        send_y(k, 2, own, 0).wait_recv()
        add(k, own, rows_of(k, 0), slot_y(k, 2))
        leave(k, 0)
        send_x(k, 2, own, 1).wait_recv()
        add(k, own, rows_of(k, 1), slot_x(k, 2))
        leave(k, 1)

    def line_first(n):
        @pl.when(jnp.logical_not(end))
        def _():
            for q in range(4):
                pass_on(n, q)

    def line_second():
        @pl.when(jnp.logical_not(end))
        def _():
            for q in range(4):
                across(0, 0, q, inner).wait_recv()
                add(0, order[q], line, ri.at[0, q])
                remote(acc.at[0, order[q], line], ri.at[0, q], ms.at[2, q], mr.at[0, q], outer).start()

    def line_last():
        @pl.when(end)
        def _():
            for q in range(4):
                across(0, 0, q, inner).wait_recv()
                add(3, order[q], line, ri.at[0, q])

        @pl.when(jnp.logical_not(end))
        def _():
            for q in range(4):
                inward(0, 2, q).wait_recv()
                add(3, order[q], line, ro.at[2, q])
                across(0, 1, q, inner).wait_recv()
                add(3, order[q], line, ri.at[1, q])

    start_two(0)
    start_one(1)
    lax.fori_loop(2, 4, group, 0)
    finish_plane(0)
    start_two(1)
    start_one(2)
    line_first(1)
    line_second()
    finish_plane(1)
    start_two(2)
    line_last()
    start_one(3)
    relay(1)
    finish_plane(2)
    start_two(3)
    relay(2)
    finish_plane(3)

    for n in range(2):
        for h in range(2):
            slot = jnp.where(end, n, n + 2)
            got_z(slot, h)
            add(3, own, rows_of(0, h), rz.at[slot, h])
    outs = []
    for h in range(2):
        part = pl.ds(h * half, half)
        acc[3, own, part] = acc[3, own, part] * (1.0 / 32.0)
        o = pltpu.make_async_copy(acc.at[3, own, part], out_ref.at[part], osem.at[h])
        o.start()
        outs.append(o)
    for s in range(15):
        kind, i = ("xi", s) if s < 2 else ("dm", s - 2) if s < 6 else ("xm", s - 6) if s < 14 else ("do", 0)
        there(kind, i).wait_send()
    for k in range(4):
        for i in range(3):
            send_x(k, i, own, 0).wait_send()
            send_y(k, i, own, 0).wait_send()
    for k in range(3):
        for h in range(2):
            send_z(k, h).wait_send()

    @pl.when(end)
    def _():
        for n in range(3):
            for q in range(4):
                inward(0, n, q).wait_send()

    @pl.when(jnp.logical_not(end))
    def _():
        for q in range(4):
            for n in range(2):
                across(0, n, q, inner).wait_send()
            remote(acc.at[0, order[q], line], ri.at[0, q], ms.at[2, q], mr.at[0, q], outer).wait_send()

    for o in outs:
        o.wait()


def reduce_gradients(x_in, dy_mid, x_mid, dy_out):
    bf, f32 = jnp.bfloat16, jnp.float32
    rows = 2 * x_in.shape[0]
    dma = pltpu.SemaphoreType.DMA
    any_spec = pl.BlockSpec(memory_space=pl.ANY)
    return pl.pallas_call(
        reduce_kernel,
        out_shape=jax.ShapeDtypeStruct((512, 512), f32),
        in_specs=[any_spec] * 4,
        out_specs=any_spec,
        scratch_shapes=[
            pltpu.VMEM((2, rows, 512), bf), pltpu.VMEM((4, rows, 512), bf), pltpu.VMEM((8, rows, 512), bf), pltpu.VMEM((rows, 512), bf),
            pltpu.VMEM((4, 4, 512, 512), f32), pltpu.VMEM((3, 3, PLANE, 512), f32), pltpu.VMEM((3, 3, PLANE, 512), f32),
            pltpu.VMEM((3, 256, 512), f32), pltpu.VMEM((3, 256, 512), f32), pltpu.VMEM((4, 2, PLANE, 512), f32),
            pltpu.VMEM((3, 4, LINE, 512), f32), pltpu.VMEM((2, 4, LINE, 512), f32),
            dma((15,)), dma((15,)), dma((15,)), dma((4, 3)), dma((4, 3)), dma((4, 3)), dma((4, 3)), dma((3, 2)), dma((4, 2)),
            dma((3, 4)), dma((3, 4)), dma((3, 4)), dma((2, 4)), dma((2,)),
        ],
        compiler_params=pltpu.CompilerParams(collective_id=0, has_side_effects=True, vmem_limit_bytes=67043328),
        name="reduce",
    )(x_in, dy_mid, x_mid, dy_out)


def gather_kernel(grad_in, rl_in, rr_in, sq_in, mom_in, sl_in, sr_in, w1_in, w2_in, new_left, new_right, new_sq, new_mom, w,
                  buf, grad, rl, rr, pre, isem, zs, zr, xs, xr, ys, yr, xds, xdr, yds, ydr, cs, cr, ls, lr, lcs, lcr):
    z, y, x, c = coords()
    xp, yp, cp = dev(z, y, 1 - x, c), dev(z, 1 - y, x, c), dev(z, y, x, 1 - c)

    pairs = [(grad_in, grad), (rl_in, rl), (rr_in, rr), (sq_in, new_sq), (mom_in, new_mom), (sl_in, new_left), (sr_in, new_right), (w2_in, w.at[pl.ds(4096, 4096)])]
    pairs += [(w1_in.at[:, pl.ds(1024 * n, 1024)], w.at[pl.ds(1024 * n, 1024)]) for n in range(4)]
    loads = [pltpu.make_async_copy(src, dst, isem.at[i]) for i, (src, dst) in enumerate(pairs)]
    for load in loads[:5]:
        load.start()
    greet_signal(z, y, x, c)

    own = y * 2 + x
    for load in loads[:4]:
        load.wait()
    for load in loads[5:]:
        load.start()
    pre[...] = mm3(rl[...], grad[...])
    rl[...] = mm3(pre[...], rr[...])

    def strip_of(i):
        return pl.ds(pl.multiple_of(i * 64, 64), 64)

    def norms(i, sums):
        r = pl.ds(pl.multiple_of(i * 16, 16), 16)
        g, p = grad[r], rl[r]
        sq = STAT_DECAY * new_sq[r] + (1.0 - STAT_DECAY) * g * g
        new_sq[r] = sq
        h = g / (jnp.sqrt(sq / BIAS_CORR) + GRAFT_EPS)
        return sums[0] + h * h, sums[1] + p * p

    zero = jnp.zeros((16, 512), jnp.float32)
    graft_sq_sum, pre_sq_sum = lax.fori_loop(0, 32, norms, (zero, zero))
    graft_sum, pre_sum = jnp.sum(graft_sq_sum), jnp.sum(pre_sq_sum)
    loads[4].wait()
    ones = jnp.ones((64, 512), jnp.float32)
    scale = jnp.sqrt(graft_sum * ones) / jnp.sqrt(pre_sum * ones)

    def momentum_step(i, _):
        r = strip_of(i)
        mom = MOM_DECAY * new_mom[r] + rl[r] * scale
        new_mom[r] = mom
        buf[z, own, c, r] = mom.astype(jnp.bfloat16)
        return 0

    lax.fori_loop(0, 8, momentum_step, 0)
    greet_wait()

    low = z < 2
    end = (z == 0) | (z == 3)
    middle = jnp.logical_not(end)
    near = [jnp.where(end, n, m) for n, m in ((1, 0), (2, 2), (3, 3))]
    zb = [z] + [jnp.where(low, n, 3 - n) for n in near]
    inner = dev(jnp.where(low, z + 1, z - 1), y, x, c)
    outer = dev(jnp.where(low, 0, 3), y, x, c)
    yx = [own, (1 - y) * 2 + x, y * 2 + 1 - x, (1 - y) * 2 + 1 - x]
    line = pl.ds(2 * GATHER_PLANE, GATHER_LINE)

    def step(zk, n, cb, first, count):
        b = (zk * 4 + n) * 2 + cb
        upper = zk < 2
        col = jnp.where(upper, b % 8, b % 2)
        row = jnp.where(upper, (col // 2) * 2 + b // 8, 8 + (b - 16) // 2)

        def strip(i, _):
            at = first + i * 32
            r = pl.ds(pl.multiple_of(row * 512 + at, 32), 32)
            cc = pl.ds(pl.multiple_of((col % 2) * 512, 512), 512)
            old = w[r, cc]
            d = buf[zk, n, cb, pl.ds(pl.multiple_of(at, 32), 32), :].astype(jnp.float32)
            w[r, cc] = old - LEARN_RATE * (d + WEIGHT_DECAY * old)
            return 0

        lax.fori_loop(0, count, strip, 0)

    def plane_rows(k):
        return 512 if k == 0 else 2 * GATHER_PLANE

    def same(zk, n, where, ss, rs, peer):
        ref = buf.at[zk, n, c, where]
        return remote(ref, ref, ss, rs, peer)

    def halves(k, n, sems, peer):
        rows = plane_rows(k) // 2
        return [same(zb[k], n, pl.ds(h * rows, rows), sems[0].at[k, h], sems[1].at[k, h], peer) for h in range(2)]

    def xcopy(k, n):
        return halves(k, n, (xs, xr), xp)

    def ycopy(k, n):
        return halves(k, n, (ys, yr), yp)

    def send_plane(k):
        across, down = xcopy(k, own), ycopy(k, own)
        across[1].start()
        down[0].start()
        across[0].start()
        down[1].start()

    def xdiag(k, n):
        return same(zb[k], n, pl.ds(0, plane_rows(k) // 2), xds.at[k], xdr.at[k], xp)

    def ydiag(k, n):
        return same(zb[k], n, pl.ds(plane_rows(k) // 2, plane_rows(k) // 2), yds.at[k], ydr.at[k], yp)

    def ccopy(k, i, n):
        return same(zb[k], n, pl.ds(0, plane_rows(k)), cs.at[k, i], cr.at[k, i], cp)

    def zcopy(layer, n, peer):
        return same(layer, own, pl.ds(0, 2 * GATHER_PLANE), zs.at[n], zr.at[layer], peer)

    def zpass(k):
        return zcopy(zb[k], k + 1, inner if k == 1 else outer)

    def zown():
        return zcopy(z, 0, inner), zcopy(z, 1, outer)

    def lines(layer, ss, rs, peer):
        ref = buf.at[layer, :, c, line]
        return remote(ref, ref, ss, rs, peer)

    def forward(k):
        return lines(zb[k], ls.at[k + 1], lr.at[zb[k]], inner if k == 1 else outer)

    def line_core(k):
        return lines(zb[k], lcs.at[k - 1], lcr.at[k - 1], cp)

    def start_line():
        lines(z, ls.at[0], lr.at[z], inner).start()

        @pl.when(middle)
        def _():
            lines(z, ls.at[1], lr.at[z], outer).start()

    def take_line(k, where):
        @pl.when(where)
        def _():
            forward(k).wait_recv()
            if where is middle:
                forward(k).start()
            line_core(k).start()

    def apply_line(k):
        line_core(k).wait_recv()
        for n in range(4):
            for cb in range(2):
                step(zb[k], n, cb, 2 * GATHER_PLANE, GATHER_LINE // 32)

    send_plane(0)
    to_inner, to_outer = zown()
    to_inner.start()

    @pl.when(middle)
    def _():
        to_outer.start()

    ccopy(0, 0, own).start()
    for load in loads[5:7]:
        load.wait()
    pre[...] = mm(grad[...], grad[...], ((1,), (1,)))
    rr[...] = mm(grad[...], grad[...], ((0,), (0,)))

    def stats(i, _):
        r = strip_of(i)
        new_left[r] = STAT_DECAY * new_left[r] + (1.0 - STAT_DECAY) * pre[r]
        new_right[r] = STAT_DECAY * new_right[r] + (1.0 - STAT_DECAY) * rr[r]
        return 0

    lax.fori_loop(0, 8, stats, 0)
    for load in loads[7:]:
        load.wait()

    def meet(k):
        down, across = ycopy(k, yx[1]), xcopy(k, yx[2])
        down[0].wait_recv()
        xdiag(k, yx[1]).start()
        across[1].wait_recv()
        ydiag(k, yx[2]).start()
        down[1].wait_recv()
        ccopy(k, 1, yx[1]).start()
        across[0].wait_recv()
        ccopy(k, 2, yx[2]).start()

    def begin(k):
        send_plane(k)
        ccopy(k, 0, own).start()

    def use(k):
        for i in range(3):
            step(zb[k], yx[i], c, 0, plane_rows(k) // 32)
        for i in range(3):
            ccopy(k, i, yx[i]).wait_recv()
            step(zb[k], yx[i], 1 - c, 0, plane_rows(k) // 32)

    def meet_last(k):
        xdiag(k, yx[3]).wait_recv()
        ydiag(k, yx[3]).wait_recv()
        ccopy(k, 3, yx[3]).start()

    def use_last(k):
        step(zb[k], yx[3], c, 0, plane_rows(k) // 32)
        ccopy(k, 3, yx[3]).wait_recv()
        step(zb[k], yx[3], 1 - c, 0, plane_rows(k) // 32)

    def pass_z(k):
        zpass(k).wait_recv()
        zpass(k).start()

    meet(0)

    @pl.when(end)
    def _():
        zpass(1).wait_recv()

    @pl.when(middle)
    def _():
        pass_z(1)
        pass_z(2)

    begin(1)
    use(0)
    meet_last(0)
    start_line()

    @pl.when(end)
    def _():
        zpass(2).wait_recv()

    @pl.when(middle)
    def _():
        pass_z(3)

    begin(2)
    use_last(0)
    meet(1)
    take_line(1, middle)

    @pl.when(end)
    def _():
        zpass(3).wait_recv()

    begin(3)
    take_line(2, middle)
    take_line(1, end)
    use(1)
    meet_last(1)
    meet(2)
    take_line(3, middle)
    use_last(1)
    apply_line(1)
    use(2)
    meet_last(2)
    take_line(2, end)
    use_last(2)
    apply_line(2)
    meet(3)
    use(3)
    take_line(3, end)
    apply_line(3)
    meet_last(3)
    use_last(3)

    for k in range(4):
        for sent in xcopy(k, own) + ycopy(k, own):
            sent.wait_send()
        xdiag(k, own).wait_send()
        ydiag(k, own).wait_send()
        for i in range(4):
            ccopy(k, i, own).wait_send()
        if k:
            line_core(k).wait_send()
    to_inner.wait_send()
    lines(z, ls.at[0], lr.at[z], inner).wait_send()

    @pl.when(middle)
    def _():
        to_outer.wait_send()
        lines(z, ls.at[1], lr.at[z], outer).wait_send()
        for k in (1, 2, 3):
            zpass(k).wait_send()
            forward(k).wait_send()


def finish_step(grad, root_left, root_right, graft_sq, momentum, stat_left, stat_right, w_fc1, w_fc2):
    bf, f32 = jnp.bfloat16, jnp.float32
    dma = pltpu.SemaphoreType.DMA
    any_spec = pl.BlockSpec(memory_space=pl.ANY)
    vmem_spec = pl.BlockSpec(memory_space=pltpu.VMEM)
    tile = pltpu.VMEM((512, 512), f32)
    return pl.pallas_call(
        gather_kernel,
        out_shape=(tile, tile, tile, tile, pltpu.VMEM((8192, 1024), f32)),
        in_specs=[any_spec] * 9,
        out_specs=(vmem_spec,) * 5,
        scratch_shapes=[pltpu.VMEM((4, 4, 2, 512, 512), bf)] + [pltpu.VMEM((512, 512), f32)] * 4 + [dma((12,)), dma((5,)), dma((4,))] + [dma((4, 2))] * 4 + [dma((4,))] * 4 + [dma((4, 4)), dma((4, 4)), dma((5,)), dma((4,)), dma((3,)), dma((3,))],
        compiler_params=pltpu.CompilerParams(collective_id=1, has_side_effects=True, vmem_limit_bytes=26 * 2 ** 20),
        name="gather",
    )(grad, root_left, root_right, graft_sq, momentum, stat_left, stat_right, w_fc1, w_fc2)


def flush_kernel(left, right, sq, mom, w, left_out, right_out, sq_out, mom_out, w1_out, w2_out, sem):
    pairs = [(w.at[pl.ds(1024 * n, 1024)], w1_out.at[:, pl.ds(1024 * n, 1024)]) for n in range(4)]
    pairs += [(w.at[pl.ds(4096, 4096)], w2_out), (left, left_out), (right, right_out), (sq, sq_out), (mom, mom_out)]
    out = [pltpu.make_async_copy(src, dst, sem.at[i]) for i, (src, dst) in enumerate(pairs)]
    for o in out:
        o.start()
    for o in out:
        o.wait()


def flush(left, right, sq, mom, w, shape1, shape2):
    any_spec = pl.BlockSpec(memory_space=pl.ANY)
    tile = jax.ShapeDtypeStruct(left.shape, left.dtype)
    values = [pltpu.with_memory_space_constraint(v, pltpu.VMEM) for v in (left, right, sq, mom, w)]
    return pl.pallas_call(
        flush_kernel,
        out_shape=(tile, tile, tile, tile, jax.ShapeDtypeStruct(shape1, w.dtype), jax.ShapeDtypeStruct(shape2, w.dtype)),
        in_specs=[pl.BlockSpec(memory_space=pltpu.VMEM)] * 5,
        out_specs=(any_spec,) * 6,
        scratch_shapes=[pltpu.SemaphoreType.DMA((9,))],
        compiler_params=pltpu.CompilerParams(vmem_limit_bytes=2 ** 20),
        name="flush",
    )(*values)


def mm3(a, b):
    a_high, b_high = a.astype(jnp.bfloat16), b.astype(jnp.bfloat16)
    a_low = (a - a_high.astype(jnp.float32)).astype(jnp.bfloat16)
    b_low = (b - b_high.astype(jnp.float32)).astype(jnp.bfloat16)
    parts = [jnp.dot(p, q, preferred_element_type=jnp.float32) for p, q in ((a_high, b_low), (a_low, b_high), (a_high, b_high))]
    return parts[0] + parts[1] + parts[2]


def mm(a, b, dims=((1,), (0,))):
    return lax.dot_general(a, b, (dims, ((), ())), precision=lax.Precision.HIGHEST, preferred_element_type=jnp.float32)


def solution(mesh):
    def per_device(x_in, dy_mid, x_mid, dy_out, w_fc1, w_fc2, stat_left, stat_right, root_left, root_right, graft_sq, momentum):
        grad = reduce_gradients(x_in, dy_mid, x_mid, dy_out)
        done = finish_step(grad, root_left[0], root_right[0], graft_sq[0], momentum[0], stat_left[0], stat_right[0], w_fc1, w_fc2)
        new_left, new_right, new_sq, new_mom, new_w1, new_w2 = flush(*done, w_fc1.shape, w_fc2.shape)
        return new_w1, new_w2, new_left[None], new_right[None], new_sq[None], new_mom[None]

    row_spec = P('dp', None)
    rep_spec = P(None, None)
    tile_spec = P('dp', None, None)
    in_specs = (row_spec, row_spec, row_spec, row_spec, rep_spec, rep_spec, tile_spec, tile_spec, tile_spec, tile_spec, tile_spec, tile_spec)
    out_specs = (rep_spec, rep_spec, tile_spec, tile_spec, tile_spec, tile_spec)
    return jax.shard_map(per_device, mesh=mesh, in_specs=in_specs, out_specs=out_specs, check_vma=False)
```
